128 devices in a mesh: dp: 128 (over z, y, x, core).
Axes of the slice: x: 4, y: 4, z: 4, core: 2. Of those that a mesh axis runs over, the one named last changes fastest.
Arguments:
- hidden: bfloat16 [131072, 5120], P('dp'), may hold values from -24 to 24
- norm_gain: float32 [5120], replicated, may hold values from 0.25 to 4
- q_cotangent: bfloat16 [131072, 128], P('dp'), may hold values from -0.015625 to 0.015625
- head_output: bfloat16 [131072, 128], P('dp'), may hold values from -6 to 6
- out_cotangent: bfloat16 [131072, 5120], P('dp'), may hold values from -0.0625 to 0.0625
- master_q: float32 [5120, 128], P('dp'), may hold values from -0.125 to 0.125
- moment_q: float32 [5120, 128], P('dp'), may hold values from -6 to 6
- second_q: float32 [5120, 128], P('dp'), may hold values from 0.01 to 0.5
- master_o: float32 [128, 5120], P(None, 'dp'), may hold values from -0.0234375 to 0.0234375
- moment_o: float32 [128, 5120], P(None, 'dp'), may hold values from -6 to 6
- second_o: float32 [128, 5120], P(None, 'dp'), may hold values from 0.01 to 0.5
Outputs:
- q_param: bfloat16 [5120, 128], replicated
- o_param: bfloat16 [128, 5120], replicated
- master_q_new: float32 [5120, 128], P('dp')
- moment_q_new: float32 [5120, 128], P('dp')
- second_q_new: float32 [5120, 128], P('dp')
- master_o_new: float32 [128, 5120], P(None, 'dp')
- moment_o_new: float32 [128, 5120], P(None, 'dp')
- second_o_new: float32 [128, 5120], P(None, 'dp')
- grad_rms: float32 [], replicated
The draws below stay inside these ranges and needn't reach their ends.
All inputs are finite; a program needn't handle non-finite values.
Results may differ from the reference program's by a relative error of at most 0.0026.
Values may be sent and summed in bfloat16 or wider, within the bound.
A program may use at most 128 MiB of HBM per device.

```python
import math
import jax
import jax.numpy as jnp
from jax import lax

D = 5120
WIDTH = 128
STEP = 20
TOK_DEV = 1024
TOKENS = 131072
N_DP = 128


def strengthened(drawn, rng, source, target, parts, factor):
    owner, partner = [(jnp.arange(drawn.shape[axis_at]) // (drawn.shape[axis_at] // parts)).reshape([-1 if axis == axis_at else 1 for axis in range(drawn.ndim)]) for axis_at in (source, target)]
    chosen = jax.random.permutation(rng, parts)[partner]
    strong = (owner == chosen) | (owner == (partner + parts // 2) % parts)
    return jnp.where(strong, factor * drawn, drawn)


def block_levels(own_key, shape, cuts, low, high):
    gain = 1.0
    for axis_at, shards_of in cuts:
        heights = jax.random.uniform(jax.random.fold_in(jax.random.fold_in(own_key, 6), axis_at), (shards_of,), jnp.float32, low / len(cuts), high / len(cuts))
        gain = gain * jnp.repeat(jnp.exp(heights), shape[axis_at] // shards_of).reshape((-1,) + (1,) * (len(shape) - 1 - axis_at))
    return gain


def gaussian(own_key, shape, width, reach, shards=(), held_as=jnp.bfloat16):
    drawn = jax.random.normal(own_key, shape, jnp.float32) * width
    if len(shards) > 0:
        drawn = block_levels(own_key, shape, shards, -0.22, 0.18) * drawn
    return jnp.clip(drawn, min=-reach, max=reach).astype(held_as)


def heavy_noise(key, dims, spread, bound, shards, heavy, held_as=jnp.bfloat16):
    array = spread * jax.random.normal(key, dims, jnp.float32)
    if shards:
        array = array * block_levels(key, dims, shards, -0.22, 0.18)
    return jnp.clip(strengthened(array, jax.random.fold_in(key, 3), *heavy), -bound, bound).astype(held_as)


def setup_inputs(seed: int = 0) -> dict:
    streams_of = jax.random.split(jax.random.key(seed), 12)
    hidden = heavy_noise(streams_of[0], (TOKENS, D), 1.0, 24.0, ((0, 128),), (0, 1, 128, 5.5))
    norm_gain = jnp.clip(jnp.exp(jax.random.uniform(streams_of[1], (D,), jnp.float32, math.log(0.25), math.log(4.0))), 0.25, 4.0)
    q_cotangent = gaussian(streams_of[2], (TOKENS, WIDTH), TOKENS ** -0.5, 0.015625, ((0, 128),))
    head_output = gaussian(streams_of[3], (TOKENS, WIDTH), 1.0, 6.0, ((0, 128),))
    out_cotangent = heavy_noise(streams_of[4], (TOKENS, D), TOKENS ** -0.5, 0.0625, ((0, 128),), (0, 1, 128, 5.5))
    master_q = gaussian(streams_of[5], (D, WIDTH), 0.009, 0.125, ((0, 128),), jnp.float32)
    moment_q = gaussian(streams_of[6], (D, WIDTH), 0.5, 6.0, ((0, 128),), jnp.float32)
    second_q = jnp.clip(jnp.exp(math.log(0.5) - 3.912023 * jax.random.uniform(streams_of[7], (D, WIDTH), jnp.float32) ** block_levels(streams_of[7], (D, WIDTH), ((0, 128),), -0.2, 0.2)), 0.01, 0.5)
    master_o = gaussian(streams_of[8], (WIDTH, D), 0.0015, 0.0234375, ((1, 128),), jnp.float32)
    moment_o = gaussian(streams_of[9], (WIDTH, D), 0.5, 6.0, ((1, 128),), jnp.float32)
    second_o = jnp.clip(jnp.exp(math.log(0.5) - 3.912023 * jax.random.uniform(streams_of[10], (WIDTH, D), jnp.float32) ** block_levels(streams_of[10], (WIDTH, D), ((1, 128),), -0.2, 0.2)), 0.01, 0.5)
    return dict(hidden=hidden, norm_gain=norm_gain, q_cotangent=q_cotangent, head_output=head_output, out_cotangent=out_cotangent, master_q=master_q, moment_q=moment_q, second_q=second_q, master_o=master_o, moment_o=moment_o, second_o=second_o)


norm_eps = 1e-05
beta_one = 0.9
beta_two = 0.95
learn_rate = 0.001
decay_rate = 0.1
adam_eps = 1e-08
clip_rms = 1.0

def normalize(hidden_block, norm_gain):
    hidden_wide = hidden_block.astype(jnp.float32)
    inverse = lax.rsqrt(lax.optimization_barrier(jnp.mean(hidden_wide * hidden_wide, axis=1, keepdims=True)) + norm_eps)
    return (hidden_wide * inverse * norm_gain[None, :]).astype(jnp.bfloat16)

def adamw(master, moment, second, gradient, factor):
    clipped = gradient * factor
    moment_new = beta_one * moment + (1.0 - beta_one) * clipped
    second_new = beta_two * second + (1.0 - beta_two) * clipped * clipped
    first_fix = 1.0 - beta_one ** STEP
    second_fix = 1.0 - beta_two ** STEP
    update = moment_new / first_fix / (jnp.sqrt(second_new / second_fix) + adam_eps)
    master_new = master - learn_rate * (update + decay_rate * master)
    return (master_new, moment_new, second_new)

def reference(hidden, norm_gain, q_cotangent, head_output, out_cotangent, master_q, moment_q, second_q, master_o, moment_o, second_o):

    def accumulate(carry, index):
        first_row = index * TOK_DEV
        hidden_block = lax.dynamic_slice_in_dim(hidden, first_row, TOK_DEV, 0)
        query_block = lax.dynamic_slice_in_dim(q_cotangent, first_row, TOK_DEV, 0)
        head_block = lax.dynamic_slice_in_dim(head_output, first_row, TOK_DEV, 0)
        outer_block = lax.dynamic_slice_in_dim(out_cotangent, first_row, TOK_DEV, 0)
        normed = normalize(hidden_block, norm_gain)
        grad_query = carry[0] + jnp.dot(normed.T, query_block, preferred_element_type=jnp.float32)
        grad_outer = carry[1] + jnp.dot(head_block.T, outer_block, preferred_element_type=jnp.float32)
        return ((grad_query, grad_outer), None)
    initial = (jnp.zeros((D, WIDTH), jnp.float32), jnp.zeros((WIDTH, D), jnp.float32))
    totals, unused = lax.scan(accumulate, initial, jnp.arange(N_DP, dtype=jnp.int32))
    grad_query, grad_outer = totals
    total_square = jnp.sum(grad_query * grad_query) + jnp.sum(grad_outer * grad_outer)
    grad_rms = jnp.sqrt(total_square / (2.0 * D * WIDTH))
    factor = jnp.minimum(1.0, clip_rms / grad_rms)
    master_q_new, moment_q_new, second_q_new = adamw(master_q, moment_q, second_q, grad_query, factor)
    master_o_new, moment_o_new, second_o_new = adamw(master_o, moment_o, second_o, grad_outer, factor)
    q_param = master_q_new.astype(jnp.bfloat16)
    o_param = master_o_new.astype(jnp.bfloat16)
    return (q_param, o_param, master_q_new, moment_q_new, second_q_new, master_o_new, moment_o_new, second_o_new, grad_rms)
```

```python
import functools
import math

import jax
import jax.numpy as jnp
from jax import lax
from jax.experimental import pallas as pl
from jax.experimental.pallas import tpu as pltpu
from jax.sharding import Mesh
from jax.sharding import PartitionSpec as P

D = 5120
WIDTH = 128
STEP = 20
TOK = 1024
DP = ("z", "y", "x", "c")

norm_eps = 1e-05
beta_one = 0.9
beta_two = 0.95
learn_rate = 0.001
decay_rate = 0.1
adam_eps = 1e-08
clip_rms = 1.0

F32 = jnp.float32
BF16 = jnp.bfloat16
MESH = pl.DeviceIdType.MESH

Q_CUT = ((0, 2), (2, 4), (4, 5))
O_CUT = ((0, 1), (1, 3), (3, 5))
TILES = tuple(q[1] - q[0] + o[1] - o[0] for q, o in zip(Q_CUT, O_CUT))
ORDER = (("x", "y", "z"), ("y", "z", "x"), ("z", "x", "y"))

CHUNK = 640
CHUNKS = D // CHUNK
CHUNK_DEVS = CHUNK // 40
BLOCK = 128
BLOCKS = TOK // BLOCK


def put_chunk(grad, outs, cuts, after, j):
    tiles = grad.T.reshape(CHUNK_DEVS, 5, 8, WIDTH).astype(BF16)
    for k in range(3):
        lo, hi = cuts[k]
        at = TILES[k] - (hi - lo) if after else 0
        outs[k][pl.ds(j * CHUNK_DEVS, CHUNK_DEVS), at : at + hi - lo] = tiles[:, lo:hi]


def local_kernel(hidden, gain, qc, ho, oc, g_a, g_b, g_c, hbuf, obuf, qct, hot, squares, inverse, hsem, osem):
    outs = (g_a, g_b, g_c)

    def ocopy(j):
        cols = slice(j * CHUNK, (j + 1) * CHUNK)
        return pltpu.make_async_copy(oc.at[:, cols], obuf.at[:, cols], osem.at[j])

    def hcopy(b):
        rows = slice(b * BLOCK, (b + 1) * BLOCK)
        return pltpu.make_async_copy(hidden.at[rows], hbuf.at[rows], hsem.at[b])

    for j in range(CHUNKS):
        ocopy(j).start()
    for b in range(BLOCKS):
        hcopy(b).start()
    hot[...] = ho[...].astype(F32).T.astype(BF16)
    qct[...] = qc[...].astype(F32).T.astype(BF16)
    for j in range(CHUNKS):
        ocopy(j).wait()
        grad = jnp.dot(hot[...], obuf[:, j * CHUNK : (j + 1) * CHUNK], preferred_element_type=F32)
        put_chunk(grad, outs, O_CUT, True, j)
    for b in range(BLOCKS):
        hcopy(b).wait()

        def sum_rows(r, _):
            rows = pl.ds(pl.multiple_of(b * BLOCK + r * 16, 16), 16)
            acc = [jnp.zeros((16, 128), F32) for _ in range(4)]
            for t in range(40):
                wide = hbuf[rows, t * 128 : (t + 1) * 128].astype(F32)
                acc[t % 4] = acc[t % 4] + wide * wide
            squares[rows, :] = (acc[0] + acc[1]) + (acc[2] + acc[3])
            return 0

        lax.fori_loop(0, BLOCK // 16, sum_rows, 0)
        block = slice(b * BLOCK, (b + 1) * BLOCK)
        mean = jnp.sum(squares[block, :], axis=1, keepdims=True) * (1.0 / D)
        inverse[block, :] = jnp.broadcast_to(lax.rsqrt(mean + norm_eps), (BLOCK, 128))

        def scale_rows(r, _):
            rows = pl.ds(pl.multiple_of(b * BLOCK + r * 16, 16), 16)
            inv = inverse[rows, :]
            for t in range(40):
                cols = slice(t * 128, (t + 1) * 128)
                wide = hbuf[rows, cols].astype(F32)
                hbuf[rows, cols] = (wide * inv * gain[:, cols]).astype(BF16)
            return 0

        lax.fori_loop(0, BLOCK // 16, scale_rows, 0)
    for j in range(CHUNKS):
        grad = jnp.dot(qct[...], hbuf[:, j * CHUNK : (j + 1) * CHUNK], preferred_element_type=F32)
        put_chunk(grad, outs, Q_CUT, False, j)


def local_grads(hidden, gain, qc, ho, oc):
    vmem = pl.BlockSpec(memory_space=pltpu.VMEM)
    hbm = pl.BlockSpec(memory_space=pl.ANY)
    return pl.pallas_call(
        local_kernel,
        out_shape=[jax.ShapeDtypeStruct((128, t, 8, 128), BF16) for t in TILES],
        in_specs=[hbm, vmem, vmem, vmem, hbm],
        out_specs=[vmem] * 3,
        scratch_shapes=[
            pltpu.VMEM((TOK, D), BF16),
            pltpu.VMEM((TOK, D), BF16),
            pltpu.VMEM((128, TOK), BF16),
            pltpu.VMEM((128, TOK), BF16),
            pltpu.VMEM((TOK, 128), F32),
            pltpu.VMEM((TOK, 128), F32),
            pltpu.SemaphoreType.DMA((BLOCKS,)),
            pltpu.SemaphoreType.DMA((CHUNKS,)),
        ],
        compiler_params=pltpu.CompilerParams(vmem_limit_bytes=48 * 1024 * 1024),
        cost_estimate=pl.CostEstimate(flops=4 * TOK * D * 128, bytes_accessed=4 * TOK * D, transcendentals=0),
        name="local_grads",
    )(hidden, gain, qc, ho, oc)


def adamw(master, moment, second, gradient, factor):
    clipped = gradient * factor
    moment_new = beta_one * moment + (1.0 - beta_one) * clipped
    second_new = beta_two * second + (1.0 - beta_two) * clipped * clipped
    first_fix = 1.0 - beta_one**STEP
    second_fix = 1.0 - beta_two**STEP
    update = moment_new / first_fix / (jnp.sqrt(second_new / second_fix) + adam_eps)
    master_new = master - learn_rate * (update + decay_rate * master)
    return (master_new, moment_new, second_new)


def pick(ref, axis, index):
    return ref.at[tuple([slice(None)] * axis + [index])]


def exchange_kernel(*refs):
    g = refs[0:3]
    states = refs[3:9]
    q_out, o_out = refs[9:11]
    news = refs[11:17]
    rms_out = refs[17]
    scratch = refs[18:]
    r0, s0, r1, s1, r2, s2, r3, pp = [scratch[3 * i : 3 * i + 3] for i in range(8)]
    n0, n1, n2, n3, sem0, semr, semn0, semn, sema, sema0 = scratch[24:]

    me = {a: lax.axis_index(a) for a in DP}

    def peer(axis, j):
        size = 2 if axis == "c" else 4
        to = dict(me)
        to[axis] = lax.rem(me[axis] + j, size)
        return tuple(to[a] for a in DP)

    def remote(src, dst, sems, axis, j):
        return pltpu.make_async_remote_copy(
            src_ref=src, dst_ref=dst, send_sem=sems.at[0], recv_sem=sems.at[1],
            device_id=peer(axis, j), device_id_type=MESH,
        )

    barrier = pltpu.get_barrier_semaphore()
    pl.semaphore_signal(barrier, inc=1, device_id=peer("c", 1), device_id_type=MESH)
    for axis in "zyx":
        for j in (1, 2, 3):
            pl.semaphore_signal(barrier, inc=1, device_id=peer(axis, j), device_id_type=MESH)
    pl.semaphore_wait(barrier, 10)

    sends = []

    other = 1 - me["c"]
    first = []
    for k in range(3):
        copy = remote(g[k].at[:, :, :, other], r0[k], sem0.at[k], "c", 1)
        copy.start()
        first.append(copy)
        sends.append(copy)
    second = [[], [], []]
    for k in range(3):
        first[k].wait_recv()

        def add0(i, _, k=k):
            z, y = i // 4, lax.rem(i, 4)
            s0[k][z, y] = (g[k][z, y, :, me["c"]].astype(F32) + r0[k][z, y].astype(F32)).astype(BF16)
            return 0

        lax.fori_loop(0, 16, add0, 0)
        axis = ORDER[k][0]
        place = "zyx".index(axis)
        for j in (1, 2, 3):
            src = pick(s0[k], place, lax.rem(me[axis] + j, 4))
            copy = remote(src, r1[k].at[j - 1], semr.at[k, 0, j - 1], axis, j)
            copy.start()
            second[k].append(copy)
            sends.append(copy)
    third = [[], [], []]
    for k in range(3):
        for copy in second[k]:
            copy.wait_recv()
        axis = ORDER[k][0]
        left = "zyx".replace(axis, "")

        def add1(i, _, k=k, axis=axis):
            own = {"z": (me["z"], i), "y": (i, me["y"]), "x": (i, slice(None), me["x"])}[axis]
            total = s0[k][own].astype(F32)
            for j in range(3):
                total = total + r1[k][j, i].astype(F32)
            s1[k][i] = total.astype(BF16)
            return 0

        lax.fori_loop(0, 4, add1, 0)
        axis = ORDER[k][1]
        for j in (1, 2, 3):
            src = pick(s1[k], left.index(axis), lax.rem(me[axis] + j, 4))
            copy = remote(src, r2[k].at[j - 1], semr.at[k, 1, j - 1], axis, j)
            copy.start()
            third[k].append(copy)
            sends.append(copy)
    fourth = [[], [], []]
    for k in range(3):
        for copy in third[k]:
            copy.wait_recv()
        left = "zyx".replace(ORDER[k][0], "")
        axis = ORDER[k][1]
        own = me[axis] if left.index(axis) == 0 else (slice(None), me[axis])
        total = s1[k][own].astype(F32)
        for j in range(3):
            total = total + r2[k][j].astype(F32)
        s2[k][...] = total
        axis = ORDER[k][2]
        for j in (1, 2, 3):
            copy = remote(s2[k].at[lax.rem(me[axis] + j, 4)], r3[k].at[j - 1], semr.at[k, 2, j - 1], axis, j)
            copy.start()
            fourth[k].append(copy)
            sends.append(copy)
    grads = []
    square = jnp.zeros((8, 128), F32)
    for k in range(3):
        for copy in fourth[k]:
            copy.wait_recv()
        total = s2[k][me[ORDER[k][2]]]
        for j in range(3):
            total = total + r3[k][j]
        grads.append(total)
        square = square + jnp.sum(total * total, axis=0)

    n0[me["c"]] = square
    copy = remote(n0.at[me["c"]], n0.at[me["c"]], semn0, "c", 1)
    copy.start()
    sends.append(copy)
    copy.wait_recv()
    square = n0[0] + n0[1]
    for i, (axis, buf) in enumerate(zip("xyz", (n1, n2, n3))):
        buf[me[axis]] = square
        copies = [remote(buf.at[me[axis]], buf.at[me[axis]], semn.at[i, j - 1], axis, j) for j in (1, 2, 3)]
        for copy in copies:
            copy.start()
            sends.append(copy)
        for copy in copies:
            copy.wait_recv()
        square = (buf[0] + buf[1]) + (buf[2] + buf[3])
    total_square = jnp.sum(jnp.sum(square, axis=0, keepdims=True), axis=1, keepdims=True)
    rms = jnp.sqrt(total_square / (2.0 * D * WIDTH))
    rms_out[...] = rms
    factor = jnp.minimum(1.0, clip_rms / rms)

    here = (me["z"], me["y"], me["x"], me["c"])
    for which, cuts in enumerate((Q_CUT, O_CUT)):
        for k in range(3):
            lo, hi = cuts[k]
            at = TILES[k] - (hi - lo) if which else 0
            olds = [states[3 * which + i][lo:hi] for i in range(3)]
            fresh = adamw(*olds, grads[k][at : at + hi - lo], factor)
            for i in range(3):
                news[3 * which + i][lo:hi] = fresh[i]
            pp[k][here + (slice(at, at + hi - lo),)] = fresh[0].astype(BF16)

    waits = [None] * 3
    for step in range(3):
        for k in range(3):
            if waits[k]:
                for copy in waits[k]:
                    copy.wait_recv()
            axis = ORDER[k][2 - step]
            done = ORDER[k][3 - step :]
            index = tuple(slice(None) if a in done else me[a] for a in "zyx") + (me["c"],)
            copies = [
                remote(pp[k].at[index], pp[k].at[index], sema.at[k, step, j - 1], axis, j) for j in (1, 2, 3)
            ]
            for copy in copies:
                copy.start()
                sends.append(copy)
            waits[k] = copies
    last = []
    for k in range(3):
        for copy in waits[k]:
            copy.wait_recv()
        mine = pp[k].at[:, :, :, me["c"]]
        copy = remote(mine, mine, sema0.at[k], "c", 1)
        copy.start()
        sends.append(copy)
        last.append(copy)
    for copy in last:
        copy.wait_recv()
    for k in range(3):

        def put(i, _, k=k):
            z, y = i // 4, lax.rem(i, 4)
            whole = pp[k][z, y]
            split = Q_CUT[k][1] - Q_CUT[k][0]
            q_out[z, y, :, :, Q_CUT[k][0] : Q_CUT[k][1]] = whole[:, :, :split]
            o_out[z, y, :, :, O_CUT[k][0] : O_CUT[k][1]] = whole[:, :, split:]
            return 0

        lax.fori_loop(0, 16, put, 0)
    for copy in sends:
        copy.wait_send()


def exchange(g, states):
    vmem = pl.BlockSpec(memory_space=pltpu.VMEM)
    per = lambda lead, dtype: [pltpu.VMEM(lead + (t, 8, 128), dtype) for t in TILES]
    tile = jax.ShapeDtypeStruct((5, 8, 128), F32)
    whole = jax.ShapeDtypeStruct((4, 4, 4, 2, 5, 8, 128), BF16)
    return pl.pallas_call(
        exchange_kernel,
        out_shape=[whole, whole] + [tile] * 6 + [jax.ShapeDtypeStruct((1, 1), F32)],
        in_specs=[vmem] * 9,
        out_specs=[vmem] * 9,
        scratch_shapes=per((4, 4, 4), BF16)
        + per((4, 4, 4), BF16)
        + per((3, 4, 4), BF16)
        + per((4, 4), BF16)
        + per((3, 4), BF16)
        + per((4,), F32)
        + per((3,), F32)
        + per((4, 4, 4, 2), BF16)
        + [
            pltpu.VMEM((2, 8, 128), F32),
            pltpu.VMEM((4, 8, 128), F32),
            pltpu.VMEM((4, 8, 128), F32),
            pltpu.VMEM((4, 8, 128), F32),
            pltpu.SemaphoreType.DMA((3, 2)),
            pltpu.SemaphoreType.DMA((3, 3, 3, 2)),
            pltpu.SemaphoreType.DMA((2,)),
            pltpu.SemaphoreType.DMA((3, 3, 2)),
            pltpu.SemaphoreType.DMA((3, 3, 3, 2)),
            pltpu.SemaphoreType.DMA((3, 2)),
        ],
        compiler_params=pltpu.CompilerParams(
            collective_id=0, has_side_effects=True, vmem_limit_bytes=32 * 1024 * 1024
        ),
        name="exchange",
    )(*g, *states)


def shards(hidden, norm_gain, q_cotangent, head_output, out_cotangent, master_q, moment_q, second_q, master_o, moment_o, second_o):
    g = local_grads(hidden, norm_gain.reshape(1, D), q_cotangent, head_output, out_cotangent)
    g = [a.reshape(4, 4, 4, 2, *a.shape[1:]) for a in g]
    states = [a.reshape(5, 8, 128) for a in (master_q, moment_q, second_q, master_o.T, moment_o.T, second_o.T)]
    out = exchange(g, states)
    q_param = out[0].reshape(D, WIDTH)
    o_param = out[1].reshape(D, WIDTH).T
    fresh = [a.reshape(40, 128) for a in out[2:8]]
    return (q_param, o_param, *fresh[:3], *[a.T for a in fresh[3:]], out[8].reshape(()))


def solution(mesh):
    split = Mesh(mesh.devices.reshape(4, 4, 4, 2), DP)
    tall, wide, whole = P(DP, None), P(None, DP), P()
    return jax.shard_map(
        shards,
        mesh=split,
        in_specs=(tall, whole, tall, tall, tall, tall, tall, tall, wide, wide, wide),
        out_specs=(whole, whole, tall, tall, tall, wide, wide, wide, whole),
        check_vma=False,
    )
```

```python
import functools
import math

import jax
import jax.numpy as jnp
from jax import lax
from jax.experimental import pallas as pl
from jax.experimental.pallas import tpu as pltpu
from jax.sharding import Mesh
from jax.sharding import PartitionSpec as P

D = 5120
WIDTH = 128
STEP = 20
TOK = 1024
DP = ("z", "y", "x", "c")

norm_eps = 1e-05
beta_one = 0.9
beta_two = 0.95
learn_rate = 0.001
decay_rate = 0.1
adam_eps = 1e-08
clip_rms = 1.0

F32 = jnp.float32
BF16 = jnp.bfloat16
MESH = pl.DeviceIdType.MESH

Q_CUT = ((0, 2), (2, 4), (4, 5))
O_CUT = ((0, 1), (1, 3), (3, 5))
TILES = tuple(q[1] - q[0] + o[1] - o[0] for q, o in zip(Q_CUT, O_CUT))
ORDER = (("x", "y", "z"), ("y", "z", "x"), ("z", "x", "y"))

CHUNK = 640
CHUNKS = D // CHUNK
CHUNK_DEVS = CHUNK // 40
BLOCK = 128
BLOCKS = TOK // BLOCK


def put_chunk(grad, outs, cuts, after, j):
    tiles = grad.T.reshape(CHUNK_DEVS, 5, 8, WIDTH).astype(BF16)
    for k in range(3):
        lo, hi = cuts[k]
        at = TILES[k] - (hi - lo) if after else 0
        outs[k][pl.ds(j * CHUNK_DEVS, CHUNK_DEVS), at : at + hi - lo] = tiles[:, lo:hi]


def local_kernel(hidden, gain_hbm, qc_hbm, ho_hbm, oc, g_a, g_b, g_c, hbuf, obuf, gain, qc, ho, qct, hot, squares, inverse, hsem, osem, ssem):
    outs = (g_a, g_b, g_c)
    small = [pltpu.make_async_copy(a, b, ssem.at[i]) for i, (a, b) in enumerate(((ho_hbm, ho), (qc_hbm, qc), (gain_hbm, gain)))]
    for copy in small:
        copy.start()

    def ocopy(j):
        cols = slice(j * CHUNK, (j + 1) * CHUNK)
        return pltpu.make_async_copy(oc.at[:, cols], obuf.at[:, cols], osem.at[j])

    def hcopy(b):
        rows = slice(b * BLOCK, (b + 1) * BLOCK)
        return pltpu.make_async_copy(hidden.at[rows], hbuf.at[rows], hsem.at[b])

    for j in range(CHUNKS):
        ocopy(j).start()
    for b in range(BLOCKS):
        hcopy(b).start()
    for copy in small:
        copy.wait()
    hot[...] = ho[...].astype(F32).T.astype(BF16)
    qct[...] = qc[...].astype(F32).T.astype(BF16)
    for j in range(CHUNKS):
        ocopy(j).wait()
        grad = jnp.dot(hot[...], obuf[:, j * CHUNK : (j + 1) * CHUNK], preferred_element_type=F32)
        put_chunk(grad, outs, O_CUT, True, j)
    for b in range(BLOCKS):
        hcopy(b).wait()

        def sum_rows(r, _):
            rows = pl.ds(pl.multiple_of(b * BLOCK + r * 16, 16), 16)
            acc = [jnp.zeros((16, 128), F32) for _ in range(4)]
            for t in range(40):
                wide = hbuf[rows, t * 128 : (t + 1) * 128].astype(F32)
                acc[t % 4] = acc[t % 4] + wide * wide
            squares[rows, :] = (acc[0] + acc[1]) + (acc[2] + acc[3])
            return 0

        lax.fori_loop(0, BLOCK // 16, sum_rows, 0)
        block = slice(b * BLOCK, (b + 1) * BLOCK)
        mean = jnp.sum(squares[block, :], axis=1, keepdims=True) * (1.0 / D)
        inverse[block, :] = jnp.broadcast_to(lax.rsqrt(mean + norm_eps), (BLOCK, 128))

        def scale_rows(r, _):
            rows = pl.ds(pl.multiple_of(b * BLOCK + r * 16, 16), 16)
            inv = inverse[rows, :]
            for t in range(40):
                cols = slice(t * 128, (t + 1) * 128)
                wide = hbuf[rows, cols].astype(F32)
                hbuf[rows, cols] = (wide * inv * gain[:, cols]).astype(BF16)
            return 0

        lax.fori_loop(0, BLOCK // 16, scale_rows, 0)
    for j in range(CHUNKS):
        grad = jnp.dot(qct[...], hbuf[:, j * CHUNK : (j + 1) * CHUNK], preferred_element_type=F32)
        put_chunk(grad, outs, Q_CUT, False, j)


def local_grads(hidden, gain, qc, ho, oc):
    vmem = pl.BlockSpec(memory_space=pltpu.VMEM)
    hbm = pl.BlockSpec(memory_space=pltpu.HBM)
    return pl.pallas_call(
        local_kernel,
        out_shape=[jax.ShapeDtypeStruct((128, t, 8, 128), BF16) for t in TILES],
        in_specs=[hbm] * 5,
        out_specs=[vmem] * 3,
        scratch_shapes=[
            pltpu.VMEM((TOK, D), BF16),
            pltpu.VMEM((TOK, D), BF16),
            pltpu.VMEM((1, D), F32),
            pltpu.VMEM((TOK, 128), BF16),
            pltpu.VMEM((TOK, 128), BF16),
            pltpu.VMEM((128, TOK), BF16),
            pltpu.VMEM((128, TOK), BF16),
            pltpu.VMEM((TOK, 128), F32),
            pltpu.VMEM((TOK, 128), F32),
            pltpu.SemaphoreType.DMA((BLOCKS,)),
            pltpu.SemaphoreType.DMA((CHUNKS,)),
            pltpu.SemaphoreType.DMA((3,)),
        ],
        compiler_params=pltpu.CompilerParams(vmem_limit_bytes=48 * 1024 * 1024),
        cost_estimate=pl.CostEstimate(flops=4 * TOK * D * 128, bytes_accessed=4 * TOK * D, transcendentals=0),
        name="local_grads",
    )(hidden, gain, qc, ho, oc)


def adamw(master, moment, second, gradient, factor):
    clipped = gradient * factor
    moment_new = beta_one * moment + (1.0 - beta_one) * clipped
    second_new = beta_two * second + (1.0 - beta_two) * clipped * clipped
    first_fix = 1.0 - beta_one**STEP
    second_fix = 1.0 - beta_two**STEP
    update = moment_new / first_fix / (jnp.sqrt(second_new / second_fix) + adam_eps)
    master_new = master - learn_rate * (update + decay_rate * master)
    return (master_new, moment_new, second_new)


def pick(ref, axis, index):
    return ref.at[tuple([slice(None)] * axis + [index])]


def exchange_kernel(*refs):
    g = refs[0:3]
    states = refs[3:9]
    pp = refs[9:12]
    news, rms_out = refs[12:14]
    scratch = refs[14:]
    r0, s0, r1, s1, r2, s2, r3 = [scratch[3 * i : 3 * i + 3] for i in range(7)]
    nall, sem0, semr, semn, sema, semb, semc, semd = scratch[21:]

    me = {a: lax.axis_index(a) for a in DP}
    ring = {a: [me[a]] + [lax.rem(me[a] + j, 4) for j in (1, 2, 3)] for a in "zyx"}
    ring["c"] = [me["c"], 1 - me["c"]]
    back = {a: [me[a]] + [lax.rem(me[a] + 4 - j, 4) for j in (1, 2, 3)] for a in "zyx"}

    def peer(axis, j):
        return tuple(ring[a][j] if a == axis else me[a] for a in DP)

    def remote(src, dst, sems, axis, j):
        return pltpu.make_async_remote_copy(
            src_ref=src, dst_ref=dst, send_sem=sems.at[0], recv_sem=sems.at[1],
            device_id=peer(axis, j), device_id_type=MESH,
        )

    others = [
        (ring["z"][dz], ring["y"][dy], ring["x"][dx], ring["c"][dc])
        for dz in (2, 3, 1, 0) for dy in (2, 3, 1, 0) for dx in (2, 3, 1, 0) for dc in (1, 0)
        if dz + dy + dx + dc > 0
    ]
    barrier = pltpu.get_barrier_semaphore()
    for device in others:
        pl.semaphore_signal(barrier, inc=1, device_id=device, device_id_type=MESH)
    pl.semaphore_wait(barrier, len(others))

    sends = []

    other = 1 - me["c"]
    first = []
    for k in range(3):
        copy = remote(g[k].at[:, :, :, other], r0[k], sem0.at[k], "c", 1)
        copy.start()
        first.append(copy)
        sends.append(copy)
    second = [[], [], []]
    for k in range(3):
        first[k].wait_recv()

        def add0(i, _, k=k):
            z, y = i // 4, lax.rem(i, 4)
            s0[k][z, y] = (g[k][z, y, :, me["c"]].astype(F32) + r0[k][z, y].astype(F32)).astype(BF16)
            return 0

        lax.fori_loop(0, 16, add0, 0)
        axis = ORDER[k][0]
        place = "zyx".index(axis)
        for j in (1, 2, 3):
            src = pick(s0[k], place, ring[axis][j])
            copy = remote(src, r1[k].at[j - 1], semr.at[k, 0, j - 1], axis, j)
            copy.start()
            second[k].append(copy)
            sends.append(copy)
    third = [[], [], []]
    for k in range(3):
        for copy in second[k]:
            copy.wait_recv()
        axis = ORDER[k][0]
        left = "zyx".replace(axis, "")

        def add1(i, _, k=k, axis=axis):
            own = {"z": (me["z"], i), "y": (i, me["y"]), "x": (i, slice(None), me["x"])}[axis]
            total = s0[k][own].astype(F32)
            for j in range(3):
                total = total + r1[k][j, i].astype(F32)
            s1[k][i] = total.astype(BF16)
            return 0

        lax.fori_loop(0, 4, add1, 0)
        axis = ORDER[k][1]
        for j in (1, 2, 3):
            src = pick(s1[k], left.index(axis), ring[axis][j])
            copy = remote(src, r2[k].at[j - 1], semr.at[k, 1, j - 1], axis, j)
            copy.start()
            third[k].append(copy)
            sends.append(copy)
    fourth = [[], [], []]
    for k in range(3):
        for copy in third[k]:
            copy.wait_recv()
        left = "zyx".replace(ORDER[k][0], "")
        axis = ORDER[k][1]
        own = me[axis] if left.index(axis) == 0 else (slice(None), me[axis])
        total = s1[k][own].astype(F32)
        for j in range(3):
            total = total + r2[k][j].astype(F32)
        s2[k][...] = total
        axis = ORDER[k][2]
        for j in (1, 2, 3):
            copy = remote(s2[k].at[ring[axis][j]], r3[k].at[j - 1], semr.at[k, 2, j - 1], axis, j)
            copy.start()
            fourth[k].append(copy)
            sends.append(copy)
    grads = []
    square = jnp.zeros((8, 128), F32)
    for k in range(3):
        for copy in fourth[k]:
            copy.wait_recv()
        total = s2[k][me[ORDER[k][2]]]
        for j in range(3):
            total = total + r3[k][j]
        grads.append(total)
        square = square + jnp.sum(total * total, axis=0)

    number = ((me["z"] * 4 + me["y"]) * 4 + me["x"]) * 2 + me["c"]
    mine = nall.at[pl.ds(number, 1)]
    nall[pl.ds(number, 1), :] = jnp.sum(square, axis=0, keepdims=True)
    for device in others:
        pltpu.make_async_remote_copy(
            src_ref=mine, dst_ref=mine, send_sem=semn.at[0], recv_sem=semn.at[1],
            device_id=device, device_id_type=MESH,
        ).start()
    rest = nall.at[pl.ds(0, len(others))]
    every = remote(rest, rest, semn, "c", 1)
    every.wait_recv()
    square = nall[...]
    total_square = jnp.sum(jnp.sum(square, axis=0, keepdims=True), axis=1, keepdims=True)
    rms = jnp.sqrt(total_square / (2.0 * D * WIDTH))
    rms_out[...] = rms
    factor = jnp.minimum(1.0, clip_rms / rms)

    here = (me["z"], me["y"], me["x"], me["c"])
    for k in range(3):
        for which, cuts in enumerate((Q_CUT, O_CUT)):
            lo, hi = cuts[k]
            at = TILES[k] - (hi - lo) if which else 0
            olds = [states[3 * which + i][lo:hi] for i in range(3)]
            fresh = adamw(*olds, grads[k][at : at + hi - lo], factor)
            for i in range(3):
                news[3 * which + i, lo:hi] = fresh[i]
            pp[k][here + (slice(at, at + hi - lo),)] = fresh[0].astype(BF16)

    def block(k, i, j, every=True):
        one, two, three = ORDER[k]
        index = dict(me)
        index[one], index[two] = back[one][i], back[two][j]
        if every:
            index[three] = slice(None)
        return pp[k].at[tuple(index[a] for a in DP)]

    along3, along2, along1, cross = [{} for _ in range(4)]

    def go(kept, key, ref, sems, axis, j):
        kept[key] = remote(ref, ref, sems, axis, j)
        kept[key].start()
        sends.append(kept[key])

    near = (1, 3, 2)
    for k in range(3):
        for j in near:
            go(along3, (k, j), block(k, 0, 0, False), sema.at[k, j - 1], ORDER[k][2], j)
    for k in range(3):
        for j in near:
            along3[k, j].wait_recv()
        for j in near:
            go(along2, (k, j), block(k, 0, 0), semb.at[k, j - 1], ORDER[k][1], j)
        for j in near:
            go(along1, (k, 0, j), block(k, 0, 0), semc.at[k, 0, j - 1], ORDER[k][0], j)
        go(cross, (k, 0, 0), block(k, 0, 0), semd.at[k, 0, 0], "c", 1)
    for two in near:
        for k in range(3):
            along2[k, two].wait_recv()
            for j in near:
                go(along1, (k, two, j), block(k, 0, two), semc.at[k, two, j - 1], ORDER[k][0], j)
            go(cross, (k, 0, two), block(k, 0, two), semd.at[k, 0, two], "c", 1)
    for two in (0,) + near:
        for j in near:
            for k in range(3):
                along1[k, two, j].wait_recv()
                go(cross, (k, j, two), block(k, j, two), semd.at[k, j, two], "c", 1)
    for copy in cross.values():
        copy.wait_recv()
    every.wait_send()
    for copy in sends:
        copy.wait_send()


def exchange(g, states):
    vmem = pl.BlockSpec(memory_space=pltpu.VMEM)
    per = lambda lead, dtype: [pltpu.VMEM(lead + (t, 8, 128), dtype) for t in TILES]
    return pl.pallas_call(
        exchange_kernel,
        out_shape=[jax.ShapeDtypeStruct((4, 4, 4, 2, t, 8, 128), BF16) for t in TILES]
        + [jax.ShapeDtypeStruct((6, 5, 8, 128), F32), jax.ShapeDtypeStruct((1, 1), F32)],
        in_specs=[vmem] * 9,
        out_specs=[vmem] * 5,
        scratch_shapes=per((4, 4, 4), BF16)
        + per((4, 4, 4), BF16)
        + per((3, 4, 4), BF16)
        + per((4, 4), BF16)
        + per((3, 4), BF16)
        + per((4,), F32)
        + per((3,), F32)
        + [
            pltpu.VMEM((128, 128), F32),
            pltpu.SemaphoreType.DMA((3, 2)),
            pltpu.SemaphoreType.DMA((3, 3, 3, 2)),
            pltpu.SemaphoreType.DMA((2,)),
            pltpu.SemaphoreType.DMA((3, 3, 2)),
            pltpu.SemaphoreType.DMA((3, 3, 2)),
            pltpu.SemaphoreType.DMA((3, 4, 3, 2)),
            pltpu.SemaphoreType.DMA((3, 4, 4, 2)),
        ],
        compiler_params=pltpu.CompilerParams(
            collective_id=0, has_side_effects=True, vmem_limit_bytes=32 * 1024 * 1024
        ),
        name="exchange",
    )(*g, *states)


GROUP = 16


def finish_kernel(p_a, p_b, p_c, news, rms, q_out, o_out, *rest):
    outs, rms_out = rest[:6], rest[6]
    turned, qsem, nsem, osem = rest[7:]
    pp = (p_a, p_b, p_c)
    copies = []

    def go(src, dst, sem):
        copies.append(pltpu.make_async_copy(src, dst, sem))
        copies[-1].start()

    for k in range(3):
        lo, hi = Q_CUT[k]
        go(pp[k].at[:, 0 : hi - lo], q_out.at[:, lo:hi], qsem.at[k])
    for i in range(6):
        go(news.at[i], outs[i], nsem.at[i])
    rms_out[...] = rms[...]
    where = {}
    for k in range(3):
        lo, hi = O_CUT[k]
        for t in range(lo, hi):
            where[t] = (k, TILES[k] - hi + t)
    for group in range(128 // GROUP):
        for b in range(5):
            tiles = []
            for i in range(16):
                flat = b * 16 + i
                k, t = where[flat % 5]
                tiles.append(pp[k][group * GROUP + flat // 5, t].astype(F32))
            wide = jnp.concatenate(tiles, axis=0).T
            at = group * 640 + b * 128
            turned[:, at : at + 128] = wide.astype(BF16)
        cols = slice(group * 640, (group + 1) * 640)
        go(turned.at[:, cols], o_out.at[:, cols], osem.at[group])
    for copy in copies:
        copy.wait()


def finish(pp, news, rms):
    vmem = pl.BlockSpec(memory_space=pltpu.VMEM)
    hbm = pl.BlockSpec(memory_space=pltpu.HBM)
    return pl.pallas_call(
        finish_kernel,
        out_shape=[jax.ShapeDtypeStruct((128, 5, 8, 128), BF16), jax.ShapeDtypeStruct((WIDTH, D), BF16)]
        + [jax.ShapeDtypeStruct((5, 8, 128), F32)] * 6
        + [jax.ShapeDtypeStruct((1, 1), F32)],
        in_specs=[vmem] * 5,
        out_specs=[hbm] * 8 + [vmem],
        scratch_shapes=[
            pltpu.VMEM((WIDTH, D), BF16),
            pltpu.SemaphoreType.DMA((3,)),
            pltpu.SemaphoreType.DMA((6,)),
            pltpu.SemaphoreType.DMA((128 // GROUP,)),
        ],
        compiler_params=pltpu.CompilerParams(vmem_limit_bytes=16 * 1024 * 1024),
        name="finish",
    )(*pp, news, rms)


def shards(hidden, norm_gain, q_cotangent, head_output, out_cotangent, master_q, moment_q, second_q, master_o, moment_o, second_o):
    g = local_grads(hidden, norm_gain.reshape(1, D), q_cotangent, head_output, out_cotangent)
    g = [a.reshape(4, 4, 4, 2, *a.shape[1:]) for a in g]
    states = [a.reshape(5, 8, 128) for a in (master_q, moment_q, second_q, master_o.T, moment_o.T, second_o.T)]
    out = exchange(g, states)
    out = finish([a.reshape(128, *a.shape[4:]) for a in out[:3]], out[3], out[4])
    fresh = [a.reshape(40, 128) for a in out[2:8]]
    return (out[0].reshape(D, WIDTH), out[1], *fresh[:3], *[a.T for a in fresh[3:]], out[8].reshape(()))


def solution(mesh):
    split = Mesh(mesh.devices.reshape(4, 4, 4, 2), DP)
    tall, wide, whole = P(DP, None), P(None, DP), P()
    return jax.shard_map(
        shards,
        mesh=split,
        in_specs=(tall, whole, tall, tall, tall, tall, tall, tall, wide, wide, wide),
        out_specs=(whole, whole, tall, tall, tall, wide, wide, wide, whole),
        check_vma=False,
    )
```

```python
import functools
import math

import jax
import jax.numpy as jnp
from jax import lax
from jax.experimental import pallas as pl
from jax.experimental.pallas import tpu as pltpu
from jax.sharding import Mesh
from jax.sharding import PartitionSpec as P

D = 5120
WIDTH = 128
STEP = 20
TOK = 1024
DP = ("z", "y", "x", "c")

norm_eps = 1e-05
beta_one = 0.9
beta_two = 0.95
learn_rate = 0.001
decay_rate = 0.1
adam_eps = 1e-08
clip_rms = 1.0

F32 = jnp.float32
BF16 = jnp.bfloat16
MESH = pl.DeviceIdType.MESH

Q_CUT = ((0, 2), (2, 4), (4, 5))
O_CUT = ((0, 1), (1, 3), (3, 5))
TILES = tuple(q[1] - q[0] + o[1] - o[0] for q, o in zip(Q_CUT, O_CUT))
ORDER = (("x", "y", "z"), ("y", "z", "x"), ("z", "x", "y"))

SPAN = 1280
HALF = SPAN // 2
BLOCK = 128
ROWS = 16


def adamw(master, moment, second, gradient, factor):
    clipped = gradient * factor
    moment_new = beta_one * moment + (1.0 - beta_one) * clipped
    second_new = beta_two * second + (1.0 - beta_two) * clipped * clipped
    first_fix = 1.0 - beta_one**STEP
    second_fix = 1.0 - beta_two**STEP
    update = moment_new / first_fix / (jnp.sqrt(second_new / second_fix) + adam_eps)
    master_new = master - learn_rate * (update + decay_rate * master)
    return (master_new, moment_new, second_new)


def step_kernel(*refs):
    hidden, gain_hbm, qc_hbm, ho_hbm, oc = refs[0:5]
    olds = refs[5:11]
    pp = refs[11:14]
    news, rms_out = refs[14:16]
    scratch = refs[16:]
    hbuf, obuf, gain, qc, ho, qct, hot, states = scratch[0:8]
    full, got, half_sum = scratch[8:10], scratch[10:12], scratch[12:14]
    r1, s1, s1h, r2, s2, r3 = [scratch[14 + 3 * i : 17 + 3 * i] for i in range(6)]
    nall, hsem, osem, ssem, sem0, sem1, semr, semn, sema, semb, semc, semd = scratch[32:]

    me = {a: lax.axis_index(a) for a in DP}
    ring = {a: [me[a]] + [lax.rem(me[a] + j, 4) for j in (1, 2, 3)] for a in "zyx"}
    ring["c"] = [me["c"], 1 - me["c"]]
    back = {a: [me[a]] + [lax.rem(me[a] + 4 - j, 4) for j in (1, 2, 3)] for a in "zyx"}

    def peer(axis, j):
        return tuple(ring[a][j] if a == axis else me[a] for a in DP)

    def remote(src, dst, sems, axis, j):
        return pltpu.make_async_remote_copy(
            src_ref=src, dst_ref=dst, send_sem=sems.at[0], recv_sem=sems.at[1],
            device_id=peer(axis, j), device_id_type=MESH,
        )

    others = [
        (ring["z"][dz], ring["y"][dy], ring["x"][dx], ring["c"][dc])
        for dz in (2, 3, 1, 0) for dy in (2, 3, 1, 0) for dx in (2, 3, 1, 0) for dc in (1, 0)
        if dz + dy + dx + dc > 0
    ]
    barrier = pltpu.get_barrier_semaphore()
    for device in others:
        pl.semaphore_signal(barrier, inc=1, device_id=device, device_id_type=MESH)

    small = [
        pltpu.make_async_copy(a, b, ssem.at[i])
        for i, (a, b) in enumerate(((ho_hbm, ho), (qc_hbm, qc), (gain_hbm, gain)))
    ]
    small += [pltpu.make_async_copy(olds[i], states.at[i], ssem.at[3 + i]) for i in range(6)]
    turns = (1, 2, 3, 0)

    def columns(j, half):
        return pl.ds(pl.multiple_of(ring["z"][j] * SPAN + half * HALF, 128), HALF)

    local = []
    for copy in small[:3]:
        copy.start()
    for i in range(8):
        cols = columns(turns[i // 2], i % 2)
        rows = slice(i * BLOCK, (i + 1) * BLOCK)
        local.append(
            (
                pltpu.make_async_copy(oc.at[:, cols], obuf.at[i], osem.at[i]),
                pltpu.make_async_copy(hidden.at[rows], hbuf.at[rows], hsem.at[i]),
            )
        )
        for copy in local[-1]:
            copy.start()
    for copy in small[3:]:
        copy.start()
    for copy in small[:3]:
        copy.wait()
    hot[...] = ho[...].astype(F32).T.astype(BF16)
    qct[...] = qc[...].astype(F32).T.astype(BF16)

    sends = []
    swaps = {}
    arrive = [[], [], []]

    def swap(which, j):
        zb = ring["z"][j]
        copy = remote(full[which].at[zb, :, :, ring["c"][1]], got[which].at[zb], sem0.at[which, j], "c", 1)
        copy.start()
        swaps[which, j] = copy
        sends.append(copy)

    def spread(which, j):
        zb = ring["z"][j]
        swaps[which, j].wait_recv()
        for y in range(4):
            chip = full[which][zb, y, :, me["c"]] + got[which][zb, y]
            half_sum[which][zb, y] = chip.astype(BF16)
        for k in range(3):
            lo, hi = (Q_CUT, O_CUT)[which][k]
            at = TILES[k] - (hi - lo) if which else 0
            axis = ORDER[k][0]
            tiles, spot = slice(lo, hi), slice(at, at + hi - lo)
            if axis == "z":
                if j:
                    copy = remote(
                        half_sum[which].at[zb, :, :, tiles], r1[k].at[j - 1, :, :, spot], sem1.at[k, which, j, 0], "z", j
                    )
                    copy.start()
                    sends.append(copy)
                    arrive[k].append(copy)
            else:
                for p in (1, 3, 2):
                    to = ring[axis][p]
                    src = half_sum[which].at[zb, :, to, tiles] if axis == "x" else half_sum[which].at[zb, to, :, tiles]
                    copy = remote(src, r1[k].at[p - 1, zb, :, spot], sem1.at[k, which, j, p - 1], axis, p)
                    copy.start()
                    sends.append(copy)
                    arrive[k].append(copy)

    previous = None
    for i in range(8):
        j, half = turns[i // 2], i % 2
        local[i][0].wait()
        local[i][1].wait()
        grad = jnp.dot(hot[...], obuf[i], preferred_element_type=F32)
        full[1][ring["z"][j], 2 * half : 2 * half + 2] = grad.T.reshape(2, 4, 2, 5, 8, WIDTH)
        for r in range(BLOCK // ROWS):
            rows = slice(i * BLOCK + r * ROWS, i * BLOCK + (r + 1) * ROWS)
            wide = hbuf[rows, :].astype(F32)
            mean = jnp.sum(wide * wide, axis=1, keepdims=True) * (1.0 / D)
            hbuf[rows, :] = (wide * lax.rsqrt(mean + norm_eps) * gain[...]).astype(BF16)
        if half:
            if i == 1:
                pl.semaphore_wait(barrier, len(others))
            swap(1, j)
            if previous is not None:
                spread(1, previous)
            previous = j
    for j in turns:
        cols = pl.ds(pl.multiple_of(ring["z"][j] * SPAN, 128), SPAN)
        grad = jnp.dot(qct[...], hbuf[:, cols], preferred_element_type=F32)
        full[0][ring["z"][j]] = grad.T.reshape(4, 4, 2, 5, 8, WIDTH)
        swap(0, j)
        if j == turns[0]:
            spread(1, turns[-1])
        else:
            spread(0, previous)
        previous = j
    spread(0, previous)

    third = [[], [], []]
    for k in range(3):
        for copy in arrive[k]:
            copy.wait_recv()
        axis = ORDER[k][0]
        left = "zyx".replace(axis, "")

        def add1(i, _, k=k, axis=axis):
            own = {"z": (me["z"], i), "y": (i, me["y"]), "x": (i, slice(None), me["x"])}[axis]
            mine = {"z": (me["z"], i, slice(None)), "y": (i, me["y"], slice(None)), "x": (i, slice(None), me["x"])}[axis]
            for which in range(2):
                lo, hi = (Q_CUT, O_CUT)[which][k]
                at = TILES[k] - (hi - lo) if which else 0
                total = full[which][mine + (me["c"], slice(lo, hi))] + got[which][own + (slice(None),) * (3 - len(own)) + (slice(lo, hi),)]
                for j in range(3):
                    total = total + r1[k][j, i, :, at : at + hi - lo].astype(F32)
                s1[k][i, :, at : at + hi - lo] = total
                s1h[k][i, :, at : at + hi - lo] = total.astype(BF16)
            return 0

        lax.fori_loop(0, 4, add1, 0)
        axis = ORDER[k][1]
        for j in (1, 3, 2):
            src = s1h[k].at[ring[axis][j]] if left.index(axis) == 0 else s1h[k].at[:, ring[axis][j]]
            copy = remote(src, r2[k].at[j - 1], semr.at[k, 0, j - 1], axis, j)
            copy.start()
            third[k].append(copy)
            sends.append(copy)
    fourth = [[], [], []]
    for k in range(3):
        for copy in third[k]:
            copy.wait_recv()
        left = "zyx".replace(ORDER[k][0], "")
        axis = ORDER[k][1]
        own = me[axis] if left.index(axis) == 0 else (slice(None), me[axis])
        total = s1[k][own]
        for j in range(3):
            total = total + r2[k][j].astype(F32)
        s2[k][...] = total
        axis = ORDER[k][2]
        for j in (1, 3, 2):
            copy = remote(s2[k].at[ring[axis][j]], r3[k].at[j - 1], semr.at[k, 1, j - 1], axis, j)
            copy.start()
            fourth[k].append(copy)
            sends.append(copy)
    grads = []
    square = jnp.zeros((8, 128), F32)
    for k in range(3):
        for copy in fourth[k]:
            copy.wait_recv()
        total = s2[k][me[ORDER[k][2]]]
        for j in range(3):
            total = total + r3[k][j]
        grads.append(total)
        square = square + jnp.sum(total * total, axis=0)

    number = ((me["z"] * 4 + me["y"]) * 4 + me["x"]) * 2 + me["c"]
    mine = nall.at[pl.ds(number, 1)]
    nall[pl.ds(number, 1), :] = jnp.sum(square, axis=0, keepdims=True)
    for device in others:
        pltpu.make_async_remote_copy(
            src_ref=mine, dst_ref=mine, send_sem=semn.at[0], recv_sem=semn.at[1],
            device_id=device, device_id_type=MESH,
        ).start()
    rest = nall.at[pl.ds(0, len(others))]
    every = remote(rest, rest, semn, "c", 1)
    every.wait_recv()
    square = nall[...]
    total_square = jnp.sum(jnp.sum(square, axis=0, keepdims=True), axis=1, keepdims=True)
    rms = jnp.sqrt(total_square / (2.0 * D * WIDTH))
    rms_out[...] = rms
    factor = jnp.minimum(1.0, clip_rms / rms)

    here = (me["z"], me["y"], me["x"], me["c"])
    for copy in small[3:]:
        copy.wait()
    for k in range(3):
        for which, cuts in enumerate((Q_CUT, O_CUT)):
            lo, hi = cuts[k]
            at = TILES[k] - (hi - lo) if which else 0
            prior = [states[3 * which + i, lo:hi] for i in range(3)]
            fresh = adamw(*prior, grads[k][at : at + hi - lo], factor)
            for i in range(3):
                news[3 * which + i, lo:hi] = fresh[i]
            pp[k][here + (slice(at, at + hi - lo),)] = fresh[0].astype(BF16)

    def block(k, i, j, every=True):
        one, two, three = ORDER[k]
        index = dict(me)
        index[one], index[two] = back[one][i], back[two][j]
        if every:
            index[three] = slice(None)
        return pp[k].at[tuple(index[a] for a in DP)]

    along3, along2, along1, cross = [{} for _ in range(4)]

    def go(kept, key, ref, sems, axis, j):
        kept[key] = remote(ref, ref, sems, axis, j)
        kept[key].start()
        sends.append(kept[key])

    near = (1, 3, 2)
    for k in range(3):
        for j in near:
            go(along3, (k, j), block(k, 0, 0, False), sema.at[k, j - 1], ORDER[k][2], j)
    for k in range(3):
        for j in near:
            along3[k, j].wait_recv()
        for j in near:
            go(along2, (k, j), block(k, 0, 0), semb.at[k, j - 1], ORDER[k][1], j)
        for j in near:
            go(along1, (k, 0, j), block(k, 0, 0), semc.at[k, 0, j - 1], ORDER[k][0], j)
        go(cross, (k, 0, 0), block(k, 0, 0), semd.at[k, 0, 0], "c", 1)
    for two in near:
        for k in range(3):
            along2[k, two].wait_recv()
            for j in near:
                go(along1, (k, two, j), block(k, 0, two), semc.at[k, two, j - 1], ORDER[k][0], j)
            go(cross, (k, 0, two), block(k, 0, two), semd.at[k, 0, two], "c", 1)
    for two in (0,) + near:
        for j in near:
            for k in range(3):
                along1[k, two, j].wait_recv()
                go(cross, (k, j, two), block(k, j, two), semd.at[k, j, two], "c", 1)
    for copy in cross.values():
        copy.wait_recv()
    every.wait_send()
    for copy in sends:
        copy.wait_send()


def step(operands, states):
    vmem = pl.BlockSpec(memory_space=pltpu.VMEM)
    hbm = pl.BlockSpec(memory_space=pltpu.HBM)
    per = lambda lead, dtype: [pltpu.VMEM(lead + (t, 8, 128), dtype) for t in TILES]
    dma = pltpu.SemaphoreType.DMA
    return pl.pallas_call(
        step_kernel,
        out_shape=[pltpu.VMEM((4, 4, 4, 2, t, 8, 128), BF16) for t in TILES]
        + [pltpu.VMEM((6, 5, 8, 128), F32), jax.ShapeDtypeStruct((1, 1), F32)],
        in_specs=[hbm] * 11,
        out_specs=[vmem] * 5,
        scratch_shapes=[
            pltpu.VMEM((TOK, D), BF16),
            pltpu.VMEM((8, TOK, HALF), BF16),
            pltpu.VMEM((1, D), F32),
            pltpu.VMEM((TOK, 128), BF16),
            pltpu.VMEM((TOK, 128), BF16),
            pltpu.VMEM((128, TOK), BF16),
            pltpu.VMEM((128, TOK), BF16),
            pltpu.VMEM((6, 5, 8, 128), F32),
        ]
        + [pltpu.VMEM((4, 4, 4, 2, 5, 8, 128), F32)] * 2
        + [pltpu.VMEM((4, 4, 4, 5, 8, 128), F32)] * 2
        + [pltpu.VMEM((4, 4, 4, 5, 8, 128), BF16)] * 2
        + per((3, 4, 4), BF16)
        + per((4, 4), F32)
        + per((4, 4), BF16)
        + per((3, 4), BF16)
        + per((4,), F32)
        + per((3,), F32)
        + [
            pltpu.VMEM((128, 128), F32),
            dma((8,)),
            dma((8,)),
            dma((9,)),
            dma((2, 4, 2)),
            dma((3, 2, 4, 3, 2)),
            dma((3, 2, 3, 2)),
            dma((2,)),
            dma((3, 3, 2)),
            dma((3, 3, 2)),
            dma((3, 4, 3, 2)),
            dma((3, 4, 4, 2)),
        ],
        compiler_params=pltpu.CompilerParams(
            collective_id=0, has_side_effects=True, vmem_limit_bytes=58 * 1024 * 1024
        ),
        cost_estimate=pl.CostEstimate(flops=4 * TOK * D * 128, bytes_accessed=4 * TOK * D, transcendentals=0),
        name="step",
    )(*operands, *states)


GROUP = 16


def finish_kernel(p_a, p_b, p_c, news, rms, q_out, o_out, *rest):
    outs, rms_out = rest[:6], rest[6]
    turned, qsem, nsem, osem = rest[7:]
    pp = (p_a, p_b, p_c)
    copies = []

    def go(src, dst, sem):
        copies.append(pltpu.make_async_copy(src, dst, sem))
        copies[-1].start()

    for k in range(3):
        lo, hi = Q_CUT[k]
        go(pp[k].at[:, 0 : hi - lo], q_out.at[:, lo:hi], qsem.at[k])
    for i in range(6):
        go(news.at[i], outs[i], nsem.at[i])
    rms_out[...] = rms[...]
    where = {}
    for k in range(3):
        lo, hi = O_CUT[k]
        for t in range(lo, hi):
            where[t] = (k, TILES[k] - hi + t)
    for group in range(128 // GROUP):
        for b in range(5):
            tiles = []
            for i in range(16):
                flat = b * 16 + i
                k, t = where[flat % 5]
                tiles.append(pp[k][group * GROUP + flat // 5, t].astype(F32))
            wide = jnp.concatenate(tiles, axis=0).T
            at = group * 640 + b * 128
            turned[:, at : at + 128] = wide.astype(BF16)
        cols = slice(group * 640, (group + 1) * 640)
        go(turned.at[:, cols], o_out.at[:, cols], osem.at[group])
    for copy in copies:
        copy.wait()


def finish(pp, news, rms):
    vmem = pl.BlockSpec(memory_space=pltpu.VMEM)
    hbm = pl.BlockSpec(memory_space=pltpu.HBM)
    return pl.pallas_call(
        finish_kernel,
        out_shape=[jax.ShapeDtypeStruct((128, 5, 8, 128), BF16), jax.ShapeDtypeStruct((WIDTH, D), BF16)]
        + [jax.ShapeDtypeStruct((5, 8, 128), F32)] * 6
        + [jax.ShapeDtypeStruct((1, 1), F32)],
        in_specs=[vmem] * 5,
        out_specs=[hbm] * 8 + [vmem],
        scratch_shapes=[
            pltpu.VMEM((WIDTH, D), BF16),
            pltpu.SemaphoreType.DMA((3,)),
            pltpu.SemaphoreType.DMA((6,)),
            pltpu.SemaphoreType.DMA((128 // GROUP,)),
        ],
        compiler_params=pltpu.CompilerParams(vmem_limit_bytes=16 * 1024 * 1024),
        name="finish",
    )(*pp, news, rms)


def shards(hidden, norm_gain, q_cotangent, head_output, out_cotangent, master_q, moment_q, second_q, master_o, moment_o, second_o):
    states = [a.reshape(5, 8, 128) for a in (master_q, moment_q, second_q, master_o.T, moment_o.T, second_o.T)]
    out = step((hidden, norm_gain.reshape(1, D), q_cotangent, head_output, out_cotangent), states)
    out = finish([a.reshape(128, *a.shape[4:]) for a in out[:3]], out[3], out[4])
    fresh = [a.reshape(40, 128) for a in out[2:8]]
    return (out[0].reshape(D, WIDTH), out[1], *fresh[:3], *[a.T for a in fresh[3:]], out[8].reshape(()))


def solution(mesh):
    split = Mesh(mesh.devices.reshape(4, 4, 4, 2), DP)
    tall, wide, whole = P(DP, None), P(None, DP), P()
    return jax.shard_map(
        shards,
        mesh=split,
        in_specs=(tall, whole, tall, tall, tall, tall, tall, tall, wide, wide, wide),
        out_specs=(whole, whole, tall, tall, tall, wide, wide, wide, whole),
        check_vma=False,
    )
```

```python
import functools
import math

import jax
import jax.numpy as jnp
from jax import lax
from jax.experimental import pallas as pl
from jax.experimental.pallas import tpu as pltpu
from jax.sharding import Mesh
from jax.sharding import PartitionSpec as P

D = 5120
WIDTH = 128
STEP = 20
TOK = 1024
DP = ("z", "y", "x", "c")

norm_eps = 1e-05
beta_one = 0.9
beta_two = 0.95
learn_rate = 0.001
decay_rate = 0.1
adam_eps = 1e-08
clip_rms = 1.0

F32 = jnp.float32
BF16 = jnp.bfloat16
MESH = pl.DeviceIdType.MESH

Q_CUT = ((0, 2), (2, 4), (4, 5))
O_CUT = ((0, 1), (1, 3), (3, 5))
TILES = tuple(q[1] - q[0] + o[1] - o[0] for q, o in zip(Q_CUT, O_CUT))
ORDER = (("x", "y", "z"), ("y", "z", "x"), ("z", "x", "y"))

SPAN = 1280
HALF = SPAN // 2
BLOCK = 128
ROWS = 16


def adamw(master, moment, second, gradient, factor):
    clipped = gradient * factor
    moment_new = beta_one * moment + (1.0 - beta_one) * clipped
    second_new = beta_two * second + (1.0 - beta_two) * clipped * clipped
    first_fix = 1.0 - beta_one**STEP
    second_fix = 1.0 - beta_two**STEP
    update = moment_new / first_fix / (jnp.sqrt(second_new / second_fix) + adam_eps)
    master_new = master - learn_rate * (update + decay_rate * master)
    return (master_new, moment_new, second_new)


def step_kernel(*refs):
    hidden, gain_hbm, qc_hbm, ho_hbm, oc = refs[0:5]
    olds = refs[5:11]
    pp = refs[11:14]
    news, rms_out = refs[14:16]
    scratch = refs[16:]
    hbuf, obuf, gain, qc, ho, qct, hot, states = scratch[0:8]
    full, got, half_sum = scratch[8:10], scratch[10:12], scratch[12:14]
    r1, s1, s1h, r2, s2, r3 = [scratch[14 + 3 * i : 17 + 3 * i] for i in range(6)]
    nall, hsem, osem, ssem, swap_sent, swap_got, pairs, two_got, one_got, near_sent, semn = scratch[32:]

    me = {a: lax.axis_index(a) for a in DP}
    ring = {a: [me[a]] + [lax.rem(me[a] + j, 4) for j in (1, 2, 3)] for a in "zyx"}
    ring["c"] = [me["c"], 1 - me["c"]]
    back = {a: [me[a]] + [lax.rem(me[a] + 4 - j, 4) for j in (1, 2, 3)] for a in "zyx"}

    def peer(axis, j):
        return tuple(ring[a][j] if a == axis else me[a] for a in DP)

    def remote(src, dst, sent, got_sem, axis, j):
        return pltpu.make_async_remote_copy(
            src_ref=src, dst_ref=dst, send_sem=sent, recv_sem=got_sem,
            device_id=peer(axis, j), device_id_type=MESH,
        )

    drains = []

    def whole(ref, sent, got_sem, drain=True):
        every = remote(ref, ref, sent, got_sem, "c", 1)
        if drain:
            drains.append(every)
        return every

    def pair(stage, k):
        return pairs.at[stage, k, 0], pairs.at[stage, k, 1]

    others = [
        (ring["z"][dz], ring["y"][dy], ring["x"][dx], ring["c"][dc])
        for dz in (2, 3, 1, 0) for dy in (2, 3, 1, 0) for dx in (2, 3, 1, 0) for dc in (1, 0)
        if dz + dy + dx + dc > 0
    ]
    barrier = pltpu.get_barrier_semaphore()
    for device in others:
        pl.semaphore_signal(barrier, inc=1, device_id=device, device_id_type=MESH)

    small = [
        pltpu.make_async_copy(a, b, ssem.at[i])
        for i, (a, b) in enumerate(((ho_hbm, ho), (qc_hbm, qc), (gain_hbm, gain)))
    ]
    small += [pltpu.make_async_copy(olds[i], states.at[i], ssem.at[3]) for i in range(6)]
    turns = (1, 2, 3, 0)

    def columns(j, half):
        return pl.ds(pl.multiple_of(ring["z"][j] * SPAN + half * HALF, 128), HALF)

    local = []
    for copy in small[:3]:
        copy.start()
    for i in range(8):
        cols = columns(turns[i // 2], i % 2)
        rows = slice(i * BLOCK, (i + 1) * BLOCK)
        local.append(
            (
                pltpu.make_async_copy(oc.at[:, cols], obuf.at[i], osem.at[i]),
                pltpu.make_async_copy(hidden.at[rows], hbuf.at[rows], hsem.at[i]),
            )
        )
        for copy in local[-1]:
            copy.start()
    for copy in small[3:]:
        copy.start()
    for copy in small[:3]:
        copy.wait()
    hot[...] = ho[...].astype(F32).T.astype(BF16)
    qct[...] = qc[...].astype(F32).T.astype(BF16)


    def swap(which, j):
        zb = ring["z"][j]
        src = full[which].at[zb, :, :, ring["c"][1]]
        remote(src, got[which].at[zb], swap_sent.at[which], swap_got.at[which, j], "c", 1).start()

    def spread(which, j):
        zb = ring["z"][j]
        whole(got[which].at[zb], swap_sent.at[which], swap_got.at[which, j], False).wait_recv()
        for y in range(4):
            chip = full[which][zb, y, :, me["c"]] + got[which][zb, y]
            half_sum[which][zb, y] = chip.astype(BF16)
        for k in range(3):
            lo, hi = (Q_CUT, O_CUT)[which][k]
            at = TILES[k] - (hi - lo) if which else 0
            axis = ORDER[k][0]
            tiles, spot = slice(lo, hi), slice(at, at + hi - lo)
            if axis == "z":
                if j:
                    remote(
                        half_sum[which].at[zb, :, :, tiles], r1[k].at[j - 1, :, :, spot], *pair(0, k), "z", j
                    ).start()
            else:
                for p in (1, 3, 2):
                    to = ring[axis][p]
                    src = half_sum[which].at[zb, :, to, tiles] if axis == "x" else half_sum[which].at[zb, to, :, tiles]
                    remote(src, r1[k].at[p - 1, zb, :, spot], *pair(0, k), axis, p).start()

    previous = None
    for i in range(8):
        j, half = turns[i // 2], i % 2
        local[i][0].wait()
        local[i][1].wait()
        grad = jnp.dot(hot[...], obuf[i], preferred_element_type=F32)
        full[1][ring["z"][j], 2 * half : 2 * half + 2] = grad.T.reshape(2, 4, 2, 5, 8, WIDTH)
        for r in range(BLOCK // ROWS):
            rows = slice(i * BLOCK + r * ROWS, i * BLOCK + (r + 1) * ROWS)
            wide = hbuf[rows, :].astype(F32)
            mean = jnp.sum(wide * wide, axis=1, keepdims=True) * (1.0 / D)
            hbuf[rows, :] = (wide * lax.rsqrt(mean + norm_eps) * gain[...]).astype(BF16)
        if half:
            if i == 1:
                pl.semaphore_wait(barrier, len(others))
            swap(1, j)
            if previous is not None:
                spread(1, previous)
            previous = j
    for j in turns:
        cols = pl.ds(pl.multiple_of(ring["z"][j] * SPAN, 128), SPAN)
        grad = jnp.dot(qct[...], hbuf[:, cols], preferred_element_type=F32)
        full[0][ring["z"][j]] = grad.T.reshape(4, 4, 2, 5, 8, WIDTH)
        swap(0, j)
        if j == turns[0]:
            spread(1, turns[-1])
        else:
            spread(0, previous)
        previous = j
    spread(0, previous)

    for which in range(2):
        whole(got[which], swap_sent.at[which], swap_got.at[which, 0])
    for k in range(3):
        whole(r1[k], *pair(0, k)).wait_recv()
        axis = ORDER[k][0]
        left = "zyx".replace(axis, "")

        def add1(i, _, k=k, axis=axis):
            own = {"z": (me["z"], i), "y": (i, me["y"]), "x": (i, slice(None), me["x"])}[axis]
            mine = {"z": (me["z"], i, slice(None)), "y": (i, me["y"], slice(None)), "x": (i, slice(None), me["x"])}[axis]
            for which in range(2):
                lo, hi = (Q_CUT, O_CUT)[which][k]
                at = TILES[k] - (hi - lo) if which else 0
                total = full[which][mine + (me["c"], slice(lo, hi))] + got[which][own + (slice(None),) * (3 - len(own)) + (slice(lo, hi),)]
                for j in range(3):
                    total = total + r1[k][j, i, :, at : at + hi - lo].astype(F32)
                s1[k][i, :, at : at + hi - lo] = total
                s1h[k][i, :, at : at + hi - lo] = total.astype(BF16)
            return 0

        lax.fori_loop(0, 4, add1, 0)
        axis = ORDER[k][1]
        for j in (1, 3, 2):
            src = s1h[k].at[ring[axis][j]] if left.index(axis) == 0 else s1h[k].at[:, ring[axis][j]]
            remote(src, r2[k].at[j - 1], *pair(1, k), axis, j).start()
    for k in range(3):
        whole(r2[k], *pair(1, k)).wait_recv()
        left = "zyx".replace(ORDER[k][0], "")
        axis = ORDER[k][1]
        own = me[axis] if left.index(axis) == 0 else (slice(None), me[axis])
        total = s1[k][own]
        for j in range(3):
            total = total + r2[k][j].astype(F32)
        s2[k][...] = total
        axis = ORDER[k][2]
        for j in (1, 3, 2):
            remote(s2[k].at[ring[axis][j]], r3[k].at[j - 1], *pair(2, k), axis, j).start()
    grads = []
    square = jnp.zeros((8, 128), F32)
    for k in range(3):
        whole(r3[k], *pair(2, k)).wait_recv()
        total = s2[k][me[ORDER[k][2]]]
        for j in range(3):
            total = total + r3[k][j]
        grads.append(total)
        square = square + jnp.sum(total * total, axis=0)

    number = ((me["z"] * 4 + me["y"]) * 4 + me["x"]) * 2 + me["c"]
    mine = nall.at[pl.ds(number, 1)]
    nall[pl.ds(number, 1), :] = jnp.sum(square, axis=0, keepdims=True)
    for device in others:
        pltpu.make_async_remote_copy(
            src_ref=mine, dst_ref=mine, send_sem=semn.at[0], recv_sem=semn.at[1],
            device_id=device, device_id_type=MESH,
        ).start()
    rest = nall.at[pl.ds(0, len(others))]
    whole(rest, semn.at[0], semn.at[1]).wait_recv()
    square = nall[...]
    total_square = jnp.sum(jnp.sum(square, axis=0, keepdims=True), axis=1, keepdims=True)
    rms = jnp.sqrt(total_square / (2.0 * D * WIDTH))
    rms_out[...] = rms
    factor = jnp.minimum(1.0, clip_rms / rms)

    here = (me["z"], me["y"], me["x"], me["c"])
    pltpu.make_async_copy(states, states, ssem.at[3]).wait()
    for k in range(3):
        for which, cuts in enumerate((Q_CUT, O_CUT)):
            lo, hi = cuts[k]
            at = TILES[k] - (hi - lo) if which else 0
            prior = [states[3 * which + i, lo:hi] for i in range(3)]
            fresh = adamw(*prior, grads[k][at : at + hi - lo], factor)
            for i in range(3):
                news[3 * which + i, lo:hi] = fresh[i]
            pp[k][here + (slice(at, at + hi - lo),)] = fresh[0].astype(BF16)

    def block(k, i, j, every=True):
        one, two, three = ORDER[k]
        index = dict(me)
        index[one], index[two] = back[one][i], back[two][j]
        if every:
            index[three] = slice(None)
        return pp[k].at[tuple(index[a] for a in DP)]

    def go(ref, sent, got_sem, axis, j):
        remote(ref, ref, sent, got_sem, axis, j).start()

    near = (1, 3, 2)
    for k in range(3):
        for j in near:
            go(block(k, 0, 0, False), *pair(3, k), ORDER[k][2], j)
    for k in range(3):
        whole(pp[k].at[0, 0, 0:3, 0], *pair(3, k)).wait_recv()
        mine = block(k, 0, 0)
        for j in near:
            go(mine, near_sent.at[0, k], two_got.at[k, j - 1], ORDER[k][1], j)
        for j in near:
            go(mine, near_sent.at[1, k], one_got.at[k, 0], ORDER[k][0], j)
        go(mine, *pair(4, k), "c", 1)
    for two in near:
        for k in range(3):
            theirs = block(k, 0, two)
            whole(theirs, near_sent.at[0, k], two_got.at[k, two - 1], False).wait_recv()
            for j in near:
                go(theirs, near_sent.at[1, k], one_got.at[k, two], ORDER[k][0], j)
            go(theirs, *pair(4, k), "c", 1)
    for two in (0,) + near:
        for k in range(3):
            whole(pp[k].at[0, 0:3, :, 0], near_sent.at[1, k], one_got.at[k, two], False).wait_recv()
            for j in near:
                go(block(k, j, two), *pair(4, k), "c", 1)
    for k in range(3):
        whole(pp[k].at[:, :, :, 0], *pair(4, k)).wait_recv()
        whole(pp[k].at[0, 0:3, :, 0], near_sent.at[0, k], two_got.at[k, 0])
        whole(pp[k].at[0:3, :, :, 0], near_sent.at[1, k], one_got.at[k, 0])
    for every in drains:
        every.wait_send()


def step(operands, states):
    vmem = pl.BlockSpec(memory_space=pltpu.VMEM)
    hbm = pl.BlockSpec(memory_space=pltpu.HBM)
    per = lambda lead, dtype: [pltpu.VMEM(lead + (t, 8, 128), dtype) for t in TILES]
    dma = pltpu.SemaphoreType.DMA
    return pl.pallas_call(
        step_kernel,
        out_shape=[pltpu.VMEM((4, 4, 4, 2, t, 8, 128), BF16) for t in TILES]
        + [pltpu.VMEM((6, 5, 8, 128), F32), jax.ShapeDtypeStruct((1, 1), F32)],
        in_specs=[hbm] * 11,
        out_specs=[vmem] * 5,
        scratch_shapes=[
            pltpu.VMEM((TOK, D), BF16),
            pltpu.VMEM((8, TOK, HALF), BF16),
            pltpu.VMEM((1, D), F32),
            pltpu.VMEM((TOK, 128), BF16),
            pltpu.VMEM((TOK, 128), BF16),
            pltpu.VMEM((128, TOK), BF16),
            pltpu.VMEM((128, TOK), BF16),
            pltpu.VMEM((6, 5, 8, 128), F32),
        ]
        + [pltpu.VMEM((4, 4, 4, 2, 5, 8, 128), F32)] * 2
        + [pltpu.VMEM((4, 4, 4, 5, 8, 128), F32)] * 2
        + [pltpu.VMEM((4, 4, 4, 5, 8, 128), BF16)] * 2
        + per((3, 4, 4), BF16)
        + per((4, 4), F32)
        + per((4, 4), BF16)
        + per((3, 4), BF16)
        + per((4,), F32)
        + per((3,), F32)
        + [
            pltpu.VMEM((128, 128), F32),
            dma((8,)),
            dma((8,)),
            dma((4,)),
            dma((2,)),
            dma((2, 4)),
            dma((5, 3, 2)),
            dma((3, 3)),
            dma((3, 4)),
            dma((2, 3)),
            dma((2,)),
        ],
        compiler_params=pltpu.CompilerParams(
            collective_id=0, has_side_effects=True, vmem_limit_bytes=58 * 1024 * 1024
        ),
        cost_estimate=pl.CostEstimate(flops=4 * TOK * D * 128, bytes_accessed=4 * TOK * D, transcendentals=0),
        name="step",
    )(*operands, *states)


GROUP = 16


def finish_kernel(p_a, p_b, p_c, news, rms, q_out, o_out, *rest):
    outs, rms_out = rest[:6], rest[6]
    turned, qsem, nsem, osem = rest[7:]
    pp = (p_a, p_b, p_c)
    copies = []

    def go(src, dst, sem):
        copies.append(pltpu.make_async_copy(src, dst, sem))
        copies[-1].start()

    for k in range(3):
        lo, hi = Q_CUT[k]
        go(pp[k].at[:, 0 : hi - lo], q_out.at[:, lo:hi], qsem.at[k])
    for i in range(6):
        go(news.at[i], outs[i], nsem.at[i])
    rms_out[...] = rms[...]
    where = {}
    for k in range(3):
        lo, hi = O_CUT[k]
        for t in range(lo, hi):
            where[t] = (k, TILES[k] - hi + t)
    for group in range(128 // GROUP):
        for b in range(5):
            tiles = []
            for i in range(16):
                flat = b * 16 + i
                k, t = where[flat % 5]
                tiles.append(pp[k][group * GROUP + flat // 5, t].astype(F32))
            wide = jnp.concatenate(tiles, axis=0).T
            at = group * 640 + b * 128
            turned[:, at : at + 128] = wide.astype(BF16)
        cols = slice(group * 640, (group + 1) * 640)
        go(turned.at[:, cols], o_out.at[:, cols], osem.at[group])
    for copy in copies:
        copy.wait()


def finish(pp, news, rms):
    vmem = pl.BlockSpec(memory_space=pltpu.VMEM)
    hbm = pl.BlockSpec(memory_space=pltpu.HBM)
    return pl.pallas_call(
        finish_kernel,
        out_shape=[jax.ShapeDtypeStruct((128, 5, 8, 128), BF16), jax.ShapeDtypeStruct((WIDTH, D), BF16)]
        + [jax.ShapeDtypeStruct((5, 8, 128), F32)] * 6
        + [jax.ShapeDtypeStruct((1, 1), F32)],
        in_specs=[vmem] * 5,
        out_specs=[hbm] * 8 + [vmem],
        scratch_shapes=[
            pltpu.VMEM((WIDTH, D), BF16),
            pltpu.SemaphoreType.DMA((3,)),
            pltpu.SemaphoreType.DMA((6,)),
            pltpu.SemaphoreType.DMA((128 // GROUP,)),
        ],
        compiler_params=pltpu.CompilerParams(vmem_limit_bytes=16 * 1024 * 1024),
        name="finish",
    )(*pp, news, rms)


def shards(hidden, norm_gain, q_cotangent, head_output, out_cotangent, master_q, moment_q, second_q, master_o, moment_o, second_o):
    states = [a.reshape(5, 8, 128) for a in (master_q, moment_q, second_q, master_o.T, moment_o.T, second_o.T)]
    out = step((hidden, norm_gain.reshape(1, D), q_cotangent, head_output, out_cotangent), states)
    out = finish([a.reshape(128, *a.shape[4:]) for a in out[:3]], out[3], out[4])
    fresh = [a.reshape(40, 128) for a in out[2:8]]
    return (out[0].reshape(D, WIDTH), out[1], *fresh[:3], *[a.T for a in fresh[3:]], out[8].reshape(()))


def solution(mesh):
    split = Mesh(mesh.devices.reshape(4, 4, 4, 2), DP)
    tall, wide, whole = P(DP, None), P(None, DP), P()
    return jax.shard_map(
        shards,
        mesh=split,
        in_specs=(tall, whole, tall, tall, tall, tall, tall, tall, wide, wide, wide),
        out_specs=(whole, whole, tall, tall, tall, wide, wide, wide, whole),
        check_vma=False,
    )
```

```python
import functools
import math

import jax
import jax.numpy as jnp
from jax import lax
from jax.experimental import pallas as pl
from jax.experimental.pallas import tpu as pltpu
from jax.sharding import Mesh
from jax.sharding import PartitionSpec as P

D = 5120
WIDTH = 128
STEP = 20
TOK = 1024
DP = ("z", "y", "x", "c")

norm_eps = 1e-05
beta_one = 0.9
beta_two = 0.95
learn_rate = 0.001
decay_rate = 0.1
adam_eps = 1e-08
clip_rms = 1.0

F32 = jnp.float32
BF16 = jnp.bfloat16
MESH = pl.DeviceIdType.MESH

Q_CUT = ((0, 2), (2, 4), (4, 5))
O_CUT = ((0, 1), (1, 3), (3, 5))
TILES = tuple(q[1] - q[0] + o[1] - o[0] for q, o in zip(Q_CUT, O_CUT))
ORDER = (("x", "y", "z"), ("y", "z", "x"), ("z", "x", "y"))

SPAN = 1280
HALF = SPAN // 2
BLOCK = 128
ROWS = 16


def adamw(master, moment, second, gradient, factor):
    clipped = gradient * factor
    moment_new = beta_one * moment + (1.0 - beta_one) * clipped
    second_new = beta_two * second + (1.0 - beta_two) * clipped * clipped
    first_fix = 1.0 - beta_one**STEP
    second_fix = 1.0 - beta_two**STEP
    update = moment_new / first_fix / (jnp.sqrt(second_new / second_fix) + adam_eps)
    master_new = master - learn_rate * (update + decay_rate * master)
    return (master_new, moment_new, second_new)


def step_kernel(*refs):
    hidden, gain_hbm, qc_hbm, ho_hbm, oc = refs[0:5]
    olds = refs[5:11]
    pp = refs[11:14]
    news, rms_out = refs[14:16]
    scratch = refs[16:]
    hbuf, obuf, gain, qc, ho, qct, hot, states = scratch[0:8]
    full, got, half_sum = scratch[8:10], scratch[10:12], scratch[12:14]
    r1, s1, s1h, r2 = [scratch[14 + 3 * i : 17 + 3 * i] for i in range(4)]
    nall, hsem, osem, ssem, swap_sent, swap_got, pairs, two_got, one_got, near_sent, semn = scratch[26:]

    me = {a: lax.axis_index(a) for a in DP}
    ring = {a: [me[a]] + [lax.rem(me[a] + j, 4) for j in (1, 2, 3)] for a in "zyx"}
    ring["c"] = [me["c"], 1 - me["c"]]
    back = {a: [me[a]] + [lax.rem(me[a] + 4 - j, 4) for j in (1, 2, 3)] for a in "zyx"}

    def peer(axis, j):
        return tuple(ring[a][j] if a == axis else me[a] for a in DP)

    def remote(src, dst, sent, got_sem, axis, j):
        return pltpu.make_async_remote_copy(
            src_ref=src, dst_ref=dst, send_sem=sent, recv_sem=got_sem,
            device_id=peer(axis, j), device_id_type=MESH,
        )

    drains = []

    def whole(ref, sent, got_sem, drain=True):
        every = remote(ref, ref, sent, got_sem, "c", 1)
        if drain:
            drains.append(every)
        return every

    def pair(stage, k):
        return pairs.at[stage, k, 0], pairs.at[stage, k, 1]

    others = [
        (ring["z"][dz], ring["y"][dy], ring["x"][dx], ring["c"][dc])
        for dz in (2, 3, 1, 0) for dy in (2, 3, 1, 0) for dx in (2, 3, 1, 0) for dc in (1, 0)
        if dz + dy + dx + dc > 0
    ]
    barrier = pltpu.get_barrier_semaphore()
    for device in others:
        pl.semaphore_signal(barrier, inc=1, device_id=device, device_id_type=MESH)

    small = [
        pltpu.make_async_copy(a, b, ssem.at[i])
        for i, (a, b) in enumerate(((ho_hbm, ho), (qc_hbm, qc), (gain_hbm, gain)))
    ]
    small += [pltpu.make_async_copy(olds[i], states.at[i], ssem.at[3]) for i in range(6)]
    turns = (1, 2, 3, 0)

    def columns(j, half):
        return pl.ds(pl.multiple_of(ring["z"][j] * SPAN + half * HALF, 128), HALF)

    local = []
    for copy in small[:3]:
        copy.start()
    for i in range(8):
        cols = columns(turns[i // 2], i % 2)
        rows = slice(i * BLOCK, (i + 1) * BLOCK)
        local.append(
            (
                pltpu.make_async_copy(oc.at[:, cols], obuf.at[i], osem.at[i]),
                pltpu.make_async_copy(hidden.at[rows], hbuf.at[rows], hsem.at[i]),
            )
        )
        for copy in local[-1]:
            copy.start()
    for copy in small[3:]:
        copy.start()
    for copy in small[:3]:
        copy.wait()
    hot[...] = ho[...].astype(F32).T.astype(BF16)
    qct[...] = qc[...].astype(F32).T.astype(BF16)


    def swap(which, j):
        zb = ring["z"][j]
        src = full[which].at[zb, :, :, ring["c"][1]]
        remote(src, got[which].at[zb], swap_sent.at[which], swap_got.at[which, j], "c", 1).start()

    def spread(which, j):
        zb = ring["z"][j]
        whole(got[which].at[zb], swap_sent.at[which], swap_got.at[which, j], False).wait_recv()
        for y in range(4):
            chip = full[which][zb, y, :, me["c"]] + got[which][zb, y]
            half_sum[which][zb, y] = chip.astype(BF16)
        for k in range(3):
            lo, hi = (Q_CUT, O_CUT)[which][k]
            at = TILES[k] - (hi - lo) if which else 0
            axis = ORDER[k][0]
            tiles, spot = slice(lo, hi), slice(at, at + hi - lo)
            if axis == "z":
                if j:
                    remote(
                        half_sum[which].at[zb, :, :, tiles], r1[k].at[j - 1, :, :, spot], *pair(0, k), "z", j
                    ).start()
            else:
                for p in (2, 1, 3):
                    to = ring[axis][p]
                    src = half_sum[which].at[zb, :, to, tiles] if axis == "x" else half_sum[which].at[zb, to, :, tiles]
                    remote(src, r1[k].at[p - 1, zb, :, spot], *pair(0, k), axis, p).start()

    previous = None
    for i in range(8):
        j, half = turns[i // 2], i % 2
        local[i][0].wait()
        local[i][1].wait()
        grad = jnp.dot(hot[...], obuf[i], preferred_element_type=F32)
        full[1][ring["z"][j], 2 * half : 2 * half + 2] = grad.T.reshape(2, 4, 2, 5, 8, WIDTH)
        for r in range(BLOCK // ROWS):
            rows = slice(i * BLOCK + r * ROWS, i * BLOCK + (r + 1) * ROWS)
            wide = hbuf[rows, :].astype(F32)
            mean = jnp.sum(wide * wide, axis=1, keepdims=True) * (1.0 / D)
            hbuf[rows, :] = (wide * lax.rsqrt(mean + norm_eps) * gain[...]).astype(BF16)
        if half:
            if i == 1:
                pl.semaphore_wait(barrier, len(others))
            swap(1, j)
            if previous is not None:
                spread(1, previous)
            previous = j
    for j in turns:
        cols = pl.ds(pl.multiple_of(ring["z"][j] * SPAN, 128), SPAN)
        grad = jnp.dot(qct[...], hbuf[:, cols], preferred_element_type=F32)
        full[0][ring["z"][j]] = grad.T.reshape(4, 4, 2, 5, 8, WIDTH)
        swap(0, j)
        if j == turns[0]:
            spread(1, turns[-1])
        else:
            spread(0, previous)
        previous = j
    spread(0, previous)

    for which in range(2):
        whole(got[which], swap_sent.at[which], swap_got.at[which, 0])
    for k in range(3):
        whole(r1[k], *pair(0, k)).wait_recv()
        axis = ORDER[k][0]
        left = "zyx".replace(axis, "")

        def add1(i, _, k=k, axis=axis):
            own = {"z": (me["z"], i), "y": (i, me["y"]), "x": (i, slice(None), me["x"])}[axis]
            mine = {"z": (me["z"], i, slice(None)), "y": (i, me["y"], slice(None)), "x": (i, slice(None), me["x"])}[axis]
            for which in range(2):
                lo, hi = (Q_CUT, O_CUT)[which][k]
                at = TILES[k] - (hi - lo) if which else 0
                total = full[which][mine + (me["c"], slice(lo, hi))] + got[which][own + (slice(None),) * (3 - len(own)) + (slice(lo, hi),)]
                for j in range(3):
                    total = total + r1[k][j, i, :, at : at + hi - lo].astype(F32)
                s1[k][i, :, at : at + hi - lo] = total
                s1h[k][i, :, at : at + hi - lo] = total.astype(BF16)
            return 0

        lax.fori_loop(0, 4, add1, 0)
        two, three = ORDER[k][1:]
        for j in (2, 1, 3, 0):
            for i in (2, 1, 3, 0):
                if i + j == 0:
                    continue
                at = dict(me)
                at[two], at[three] = ring[two][j], ring[three][i]
                pltpu.make_async_remote_copy(
                    src_ref=s1h[k].at[tuple(at[a] for a in left)], dst_ref=r2[k].at[4 * j + i - 1],
                    send_sem=pairs.at[1, k, 0], recv_sem=pairs.at[1, k, 1],
                    device_id=tuple(at[a] for a in DP), device_id_type=MESH,
                ).start()
    grads = []
    square = jnp.zeros((8, 128), F32)
    for k in range(3):
        whole(r2[k], *pair(1, k)).wait_recv()
        left = "zyx".replace(ORDER[k][0], "")
        total = s1[k][tuple(me[a] for a in left)]
        for n in range(15):
            total = total + r2[k][n].astype(F32)
        grads.append(total)
        square = square + jnp.sum(total * total, axis=0)

    number = ((me["z"] * 4 + me["y"]) * 4 + me["x"]) * 2 + me["c"]
    mine = nall.at[pl.ds(number, 1)]
    nall[pl.ds(number, 1), :] = jnp.sum(square, axis=0, keepdims=True)
    for device in others:
        pltpu.make_async_remote_copy(
            src_ref=mine, dst_ref=mine, send_sem=semn.at[0], recv_sem=semn.at[1],
            device_id=device, device_id_type=MESH,
        ).start()
    rest = nall.at[pl.ds(0, len(others))]
    whole(rest, semn.at[0], semn.at[1]).wait_recv()
    square = nall[...]
    total_square = jnp.sum(jnp.sum(square, axis=0, keepdims=True), axis=1, keepdims=True)
    rms = jnp.sqrt(total_square / (2.0 * D * WIDTH))
    rms_out[...] = rms
    factor = jnp.minimum(1.0, clip_rms / rms)

    here = (me["z"], me["y"], me["x"], me["c"])
    pltpu.make_async_copy(states, states, ssem.at[3]).wait()
    for k in range(3):
        for which, cuts in enumerate((Q_CUT, O_CUT)):
            lo, hi = cuts[k]
            at = TILES[k] - (hi - lo) if which else 0
            prior = [states[3 * which + i, lo:hi] for i in range(3)]
            fresh = adamw(*prior, grads[k][at : at + hi - lo], factor)
            for i in range(3):
                news[3 * which + i, lo:hi] = fresh[i]
            pp[k][here + (slice(at, at + hi - lo),)] = fresh[0].astype(BF16)

    def block(k, i, j, every=True):
        one, two, three = ORDER[k]
        index = dict(me)
        index[one], index[two] = back[one][i], back[two][j]
        if every:
            index[three] = slice(None)
        return pp[k].at[tuple(index[a] for a in DP)]

    def go(ref, sent, got_sem, axis, j):
        remote(ref, ref, sent, got_sem, axis, j).start()

    near = (1, 3, 2)
    far = (2, 1, 3)
    for k in range(3):
        share = block(k, 0, 0, False)
        for j in far:
            go(share, *pair(3, k), ORDER[k][2], j)
        for j in far:
            for i in (2, 1, 3, 0):
                at = dict(me)
                at[ORDER[k][1]], at[ORDER[k][2]] = ring[ORDER[k][1]][j], ring[ORDER[k][2]][i]
                pltpu.make_async_remote_copy(
                    src_ref=share, dst_ref=share, send_sem=near_sent.at[0, k], recv_sem=two_got.at[k, j - 1],
                    device_id=tuple(at[a] for a in DP), device_id_type=MESH,
                ).start()
    for k in range(3):
        whole(pp[k].at[0, 0, 0:3, 0], *pair(3, k)).wait_recv()
        mine = block(k, 0, 0)
        for j in far:
            go(mine, near_sent.at[1, k], one_got.at[k, 0], ORDER[k][0], j)
        go(mine, *pair(4, k), "c", 1)
    for two in near:
        for k in range(3):
            theirs = block(k, 0, two)
            whole(theirs, near_sent.at[0, k], two_got.at[k, two - 1], False).wait_recv()
            for j in far:
                go(theirs, near_sent.at[1, k], one_got.at[k, two], ORDER[k][0], j)
            go(theirs, *pair(4, k), "c", 1)
    for two in (0,) + near:
        for k in range(3):
            whole(pp[k].at[0, 0:3, :, 0], near_sent.at[1, k], one_got.at[k, two], False).wait_recv()
            for j in near:
                go(block(k, j, two), *pair(4, k), "c", 1)
    for k in range(3):
        whole(pp[k].at[:, :, :, 0], *pair(4, k)).wait_recv()
        whole(pp[k].at[0, 0:3, :, 0], near_sent.at[0, k], two_got.at[k, 0])
        whole(pp[k].at[0:3, :, :, 0], near_sent.at[1, k], one_got.at[k, 0])
    for every in drains:
        every.wait_send()


def step(operands, states):
    vmem = pl.BlockSpec(memory_space=pltpu.VMEM)
    hbm = pl.BlockSpec(memory_space=pltpu.HBM)
    per = lambda lead, dtype: [pltpu.VMEM(lead + (t, 8, 128), dtype) for t in TILES]
    dma = pltpu.SemaphoreType.DMA
    return pl.pallas_call(
        step_kernel,
        out_shape=[pltpu.VMEM((4, 4, 4, 2, t, 8, 128), BF16) for t in TILES]
        + [pltpu.VMEM((6, 5, 8, 128), F32), jax.ShapeDtypeStruct((1, 1), F32)],
        in_specs=[hbm] * 11,
        out_specs=[vmem] * 5,
        scratch_shapes=[
            pltpu.VMEM((TOK, D), BF16),
            pltpu.VMEM((8, TOK, HALF), BF16),
            pltpu.VMEM((1, D), F32),
            pltpu.VMEM((TOK, 128), BF16),
            pltpu.VMEM((TOK, 128), BF16),
            pltpu.VMEM((128, TOK), BF16),
            pltpu.VMEM((128, TOK), BF16),
            pltpu.VMEM((6, 5, 8, 128), F32),
        ]
        + [pltpu.VMEM((4, 4, 4, 2, 5, 8, 128), F32)] * 2
        + [pltpu.VMEM((4, 4, 4, 5, 8, 128), F32)] * 2
        + [pltpu.VMEM((4, 4, 4, 5, 8, 128), BF16)] * 2
        + per((3, 4, 4), BF16)
        + per((4, 4), F32)
        + per((4, 4), BF16)
        + per((15,), BF16)
        + [
            pltpu.VMEM((128, 128), F32),
            dma((8,)),
            dma((8,)),
            dma((4,)),
            dma((2,)),
            dma((2, 4)),
            dma((5, 3, 2)),
            dma((3, 3)),
            dma((3, 4)),
            dma((2, 3)),
            dma((2,)),
        ],
        compiler_params=pltpu.CompilerParams(
            collective_id=0, has_side_effects=True, vmem_limit_bytes=58 * 1024 * 1024
        ),
        cost_estimate=pl.CostEstimate(flops=4 * TOK * D * 128, bytes_accessed=4 * TOK * D, transcendentals=0),
        name="step",
    )(*operands, *states)


GROUP = 16


def finish_kernel(p_a, p_b, p_c, news, rms, q_out, o_out, *rest):
    outs, rms_out = rest[:6], rest[6]
    turned, qsem, nsem, osem = rest[7:]
    pp = (p_a, p_b, p_c)
    copies = []

    def go(src, dst, sem):
        copies.append(pltpu.make_async_copy(src, dst, sem))
        copies[-1].start()

    for k in range(3):
        lo, hi = Q_CUT[k]
        go(pp[k].at[:, 0 : hi - lo], q_out.at[:, lo:hi], qsem.at[k])
    for i in range(6):
        go(news.at[i], outs[i], nsem.at[i])
    rms_out[...] = rms[...]
    where = {}
    for k in range(3):
        lo, hi = O_CUT[k]
        for t in range(lo, hi):
            where[t] = (k, TILES[k] - hi + t)
    for group in range(128 // GROUP):
        for b in range(5):
            tiles = []
            for i in range(16):
                flat = b * 16 + i
                k, t = where[flat % 5]
                tiles.append(pp[k][group * GROUP + flat // 5, t].astype(F32))
            wide = jnp.concatenate(tiles, axis=0).T
            at = group * 640 + b * 128
            turned[:, at : at + 128] = wide.astype(BF16)
        cols = slice(group * 640, (group + 1) * 640)
        go(turned.at[:, cols], o_out.at[:, cols], osem.at[group])
    for copy in copies:
        copy.wait()


def finish(pp, news, rms):
    vmem = pl.BlockSpec(memory_space=pltpu.VMEM)
    hbm = pl.BlockSpec(memory_space=pltpu.HBM)
    return pl.pallas_call(
        finish_kernel,
        out_shape=[jax.ShapeDtypeStruct((128, 5, 8, 128), BF16), jax.ShapeDtypeStruct((WIDTH, D), BF16)]
        + [jax.ShapeDtypeStruct((5, 8, 128), F32)] * 6
        + [jax.ShapeDtypeStruct((1, 1), F32)],
        in_specs=[vmem] * 5,
        out_specs=[hbm] * 8 + [vmem],
        scratch_shapes=[
            pltpu.VMEM((WIDTH, D), BF16),
            pltpu.SemaphoreType.DMA((3,)),
            pltpu.SemaphoreType.DMA((6,)),
            pltpu.SemaphoreType.DMA((128 // GROUP,)),
        ],
        compiler_params=pltpu.CompilerParams(vmem_limit_bytes=16 * 1024 * 1024),
        name="finish",
    )(*pp, news, rms)


def shards(hidden, norm_gain, q_cotangent, head_output, out_cotangent, master_q, moment_q, second_q, master_o, moment_o, second_o):
    states = [a.reshape(5, 8, 128) for a in (master_q, moment_q, second_q, master_o.T, moment_o.T, second_o.T)]
    out = step((hidden, norm_gain.reshape(1, D), q_cotangent, head_output, out_cotangent), states)
    out = finish([a.reshape(128, *a.shape[4:]) for a in out[:3]], out[3], out[4])
    fresh = [a.reshape(40, 128) for a in out[2:8]]
    return (out[0].reshape(D, WIDTH), out[1], *fresh[:3], *[a.T for a in fresh[3:]], out[8].reshape(()))


def solution(mesh):
    split = Mesh(mesh.devices.reshape(4, 4, 4, 2), DP)
    tall, wide, whole = P(DP, None), P(None, DP), P()
    return jax.shard_map(
        shards,
        mesh=split,
        in_specs=(tall, whole, tall, tall, tall, tall, tall, tall, wide, wide, wide),
        out_specs=(whole, whole, tall, tall, tall, wide, wide, wide, whole),
        check_vma=False,
    )
```
